32 devices in a mesh: replica: 4 (over y, core), shard: 8 (over z, x).
Axes of the slice: x: 2, y: 2, z: 4, core: 2. Of those that a mesh axis runs over, the one named last changes fastest.
Arguments:
- inputs: bfloat16 [512, 2048], P('replica'), may hold values from -6 to 6
- gate_pre: bfloat16 [512, 8192], P('replica', 'shard'), may hold values from -8 to 8
- up_pre: bfloat16 [512, 8192], P('replica', 'shard'), may hold values from -6 to 6
- hidden_grad: bfloat16 [512, 8192], P('replica', 'shard'), may hold values from -6 to 6
- segment_ids: int32 [4, 128], P('replica'), may hold values from 0 to 15, never falling along the last dimension, each value on 1 to 32 neighbouring positions
- doc_weight: int32 [4, 16], P('replica'), may hold values from 1 to 12
- w_gate: bfloat16 [2048, 8192], P(None, 'shard'), may hold values from -0.0625 to 0.0625
- master: float32 [2048, 8192], P('replica', 'shard'), may hold values from -6 to 6
- moment: float32 [2048, 8192], P('replica', 'shard'), may hold values from -10 to 10
- second: float32 [2048, 8192], P('replica', 'shard'), may hold values from 0.5 to 20
Outputs:
- input_grad: bfloat16 [512, 2048], P(('replica', 'shard'))
- up_grad: bfloat16 [512, 8192], P('replica', 'shard')
- master_new: float32 [2048, 8192], P('replica', 'shard')
- moment_new: float32 [2048, 8192], P('replica', 'shard')
- second_new: float32 [2048, 8192], P('replica', 'shard')
The draws below stay inside these ranges and needn't reach their ends.
Inputs may be any that keep to these rules, and one draw needn't show every extreme that they name: `segment_ids`: within each group the documents occupy runs of positions numbered 0 to 15 in order, each at most 32 long.
All inputs are finite; a program needn't handle non-finite values.
Results may differ from the reference program's by a relative error of at most 0.0049.
Values sent between devices are 32-bit elements; how exact they have to be, the bound alone decides.
A program may use at most 64 MiB of HBM per device.

```python
import math
import jax
import jax.numpy as jnp
import numpy as np
from jax import lax

DW = 2048
FF = 8192
SEGS = 16
GROUP_TOK = 128
TOKENS = 512
N_REPLICA = 4


def draw_doc_weight(key, part):
    base_key = jax.random.fold_in(key, 11)
    start_key = jax.random.fold_in(key, 12)
    length_key = jax.random.fold_in(key, 13)
    base = jax.random.randint(base_key, (N_REPLICA, SEGS), 1, 4)
    groups = jnp.arange(N_REPLICA, dtype=jnp.int32)
    labels = jnp.arange(SEGS, dtype=jnp.int32)
    first_cell = (groups[:, None] == 0) & (labels[None, :] == 0)
    last_cell = (groups[:, None] == N_REPLICA - 1) & (labels[None, :] == 0)
    base = jnp.where(first_cell, 1, base)
    base = jnp.where(last_cell, 3, base)
    rising = 8 * groups // N_REPLICA
    window_start = jax.random.randint(start_key, (), 0, N_REPLICA)
    window_length = jax.random.randint(length_key, (), 0, N_REPLICA + 1)
    inside = (jnp.mod(groups - window_start, N_REPLICA) < window_length).astype(jnp.int32)
    inside = jnp.where(groups == 0, 0, inside)
    inside = jnp.where(groups == N_REPLICA - 1, 1, inside)
    return (base + rising[:, None] + 3 * inside[:, None]).astype(jnp.int32)


def spiked(result, stream_key, source, target, blocks, factor):
    def block_of(position):
        return (jnp.arange(result.shape[position]) // (result.shape[position] // blocks)).reshape((-1,) + (1,) * (result.ndim - 1 - position))

    one_side = jax.random.permutation(stream_key, blocks)[block_of(target)]
    other_side = (block_of(target) + blocks // 2) % blocks
    return jnp.where((block_of(source) == one_side) | (block_of(source) == other_side), factor * result, result)


def shard_levels(own_key, dims, cuts, smallest, largest):
    def one(axis_at, parts):
        steps = jax.random.uniform(jax.random.fold_in(jax.random.fold_in(own_key, 6), axis_at), (parts,), jnp.float32, smallest / len(cuts), largest / len(cuts))
        return jnp.repeat(jnp.exp(steps), dims[axis_at] // parts).reshape((-1,) + (1,) * (len(dims) - axis_at - 1))

    gain = one(*cuts[0])
    for cut in cuts[1:]:
        gain = gain * one(*cut)
    return gain


def split_up(count, total, limit, skew):
    loads = [(1 << 20) // math.isqrt(grade ** skew) + 1 for grade in range(2, count + 1)]
    surplus, holding = total - limit - (count - 1), [1] * (count - 1)
    while surplus > 0:
        free = [i for i in range(count - 1) if holding[i] < limit]
        mass, remaining = sum([loads[i] for i in free]), surplus
        for i in free:
            more = min(limit - holding[i], max(1, remaining * loads[i] // mass), surplus)
            holding[i] = holding[i] + more
            surplus = surplus - more
    return np.array([limit] + holding)


def ragged(stream_key, amount, total, bound, slope):
    if amount == 2:
        one = jax.random.randint(stream_key, (), max(1, total - bound), min(bound, total - 1) + 1)
        return jnp.stack([one, total - one])
    tallies = jnp.asarray(split_up(amount, total, bound, slope), jnp.int32)
    couples = (amount - 1) // 2
    giver, receiver = tallies[1:1 + 2 * couples:2], tallies[2:2 + 2 * couples:2]
    margin = jnp.minimum(giver - 1, bound - receiver)
    moved = jax.random.randint(jax.random.fold_in(stream_key, 1), (couples,), 0, 1 << 20) % (margin + 1)
    tallies = tallies.at[1:1 + 2 * couples:2].set(giver - moved).at[2:2 + 2 * couples:2].set(receiver + moved)
    return tallies[jax.random.permutation(jax.random.fold_in(stream_key, 2), amount)]


def noise(rng, shape, spread, reach, pieces=(), kind=jnp.bfloat16):
    loudness = shard_levels(rng, shape, pieces, -0.22, 0.18) if pieces else 1.0
    values = jax.random.normal(rng, shape, jnp.float32) * spread * loudness
    return jnp.minimum(jnp.maximum(values, -reach), reach).astype(kind)


def heavy_noise(rng, shape, deviation, limit, split, heavy, kind=jnp.bfloat16):
    drawn = deviation * jax.random.normal(rng, shape, jnp.float32)
    if split:
        drawn = drawn * shard_levels(rng, shape, split, -0.22, 0.18)
    return jnp.clip(spiked(drawn, jax.random.fold_in(rng, 3), *heavy), -limit, limit).astype(kind)


def setup_inputs(seed: int = 0) -> dict:
    keys = jax.random.split(jax.random.key(seed), 11)
    return {
        "inputs": heavy_noise(keys[0], (TOKENS, DW), 1.0, 6.0, ((0, 4),), (0, 1, 4, 2.0)),
        "gate_pre": noise(keys[1], (TOKENS, FF), 2.0, 8.0, ((0, 4), (1, 8))),
        "up_pre": noise(keys[2], (TOKENS, FF), 1.0, 6.0, ((0, 4), (1, 8))),
        "hidden_grad": heavy_noise(keys[3], (TOKENS, FF), 1.0, 6.0, ((0, 4), (1, 8)), (1, 0, 8, 2.0)),
        "segment_ids": jax.vmap(lambda own: jnp.searchsorted(jnp.cumsum(ragged(own, SEGS, GROUP_TOK, GROUP_TOK // 4, 2)), jnp.arange(GROUP_TOK), side="right"))(jax.random.split(keys[4], N_REPLICA)).reshape((N_REPLICA, GROUP_TOK)).astype(jnp.int32),
        "doc_weight": draw_doc_weight(jax.random.fold_in(keys[10], 71), 0),
        "w_gate": noise(keys[6], (DW, FF), FF ** -0.5, 0.0625, ((1, 8),)),
        "master": noise(keys[7], (DW, FF), 1.0, 6.0, ((0, 4), (1, 8)), jnp.float32),
        "moment": noise(keys[8], (DW, FF), 2.0, 10.0, ((0, 4), (1, 8)), jnp.float32),
        "second": jnp.clip(jnp.exp(math.log(20.0) - 3.6888795 * jax.random.uniform(keys[9], (DW, FF), jnp.float32) ** shard_levels(keys[9], (DW, FF), ((0, 4), (1, 8)), -0.2, 0.2)), 0.5, 20.0),
    }


def token_weights(segment_ids, doc_weight):
    labels = jnp.arange(doc_weight.shape[1], dtype=jnp.int32)
    onehot = segment_ids[:, :, None] == labels[None, None, :]
    return lax.optimization_barrier(jnp.sum(jnp.where(onehot, doc_weight[:, None, :], 0), axis=2)).astype(jnp.int32)

def reference(inputs, gate_pre, up_pre, hidden_grad, segment_ids, doc_weight, w_gate, master, moment, second):
    weights = token_weights(segment_ids, doc_weight)
    total = jnp.sum(weights).astype(jnp.int32)
    total_f = total.astype(jnp.float32)
    scale = jnp.float32(TOKENS) / total_f
    group_scale = jnp.float32(GROUP_TOK) / total_f
    stacked = (inputs.reshape(N_REPLICA, GROUP_TOK, DW), gate_pre.reshape(N_REPLICA, GROUP_TOK, FF), up_pre.reshape(N_REPLICA, GROUP_TOK, FF), hidden_grad.reshape(N_REPLICA, GROUP_TOK, FF), weights)

    def one_group(accum, block):
        rows, gate_blk, up_blk, grad_blk, weight_blk = block
        gate_f = gate_blk.astype(jnp.float32)
        sigmoid_gate = jax.nn.sigmoid(gate_f)
        weighted = grad_blk.astype(jnp.float32) * weight_blk.astype(jnp.float32)[:, None]
        gate_raw = (weighted * up_blk.astype(jnp.float32) * sigmoid_gate * (1.0 + gate_f * (1.0 - sigmoid_gate))).astype(jnp.bfloat16)
        up_out = (weighted * gate_f * sigmoid_gate * scale).astype(jnp.bfloat16)
        input_part = lax.dot_general(gate_raw, w_gate, (((1,), (1,)), ((), ())), preferred_element_type=jnp.float32)
        input_out = (input_part * scale).astype(jnp.bfloat16)
        accum = accum + lax.dot_general(rows, gate_raw, (((0,), (0,)), ((), ())), preferred_element_type=jnp.float32)
        return (accum, (input_out, up_out))
    start = jnp.zeros((DW, FF), jnp.float32)
    weight_raw, (input_grad, up_grad) = lax.scan(one_group, start, stacked)
    grad = weight_raw * group_scale
    moment_new = 0.9 * moment + 0.1 * grad
    second_new = 0.95 * second + 0.05 * grad * grad
    first_fix = moment_new / (1.0 - 0.9 ** 8)
    second_fix = second_new / (1.0 - 0.95 ** 8)
    master_new = master - 0.003 * (first_fix / (jnp.sqrt(second_fix) + 1e-08) + 0.1 * master)
    return (input_grad.reshape(TOKENS, DW), up_grad.reshape(TOKENS, FF), master_new, moment_new, second_new)
```

```python
import functools

import jax
import jax.numpy as jnp
from jax import lax
from jax.experimental import pallas as pl
from jax.experimental.pallas import tpu as pltpu
from jax.sharding import PartitionSpec as P

MESH = pl.DeviceIdType.MESH
QUARTERS = 4
CHUNKS = 4
BAND = 64
LAYOUT = (7, 3, 5, 1, 6, 2, 4, 0)
KINDS = "hmhh"
X_LAST = ("mid", "near")
DONE = 3
ORDER = (
    "p0", "p1", "p2", "c2", "xc", "b1", "p3", "st0", "st1", "st2", "st3", "x0", "a2", "c3", "c0",
    "b0", "a0", "b2", "a3", "x1", "d1", "a1", "c1", "f2", "b3", "core", "xl0", "f3", "e0", "e2",
    "own", "xl1", "f0", "e1", "g0", "g2", "f1", "scale", "d0", "g1", "d2", "d3", "e3", "t0", "t1",
    "xe0", "xe1", "opt0", "g3", "t2", "opt1", "opt2", "i1", "i0", "i2", "t3", "i3",
)


def token_weights(segment_ids, doc_weight):
    labels = jnp.arange(doc_weight.shape[1], dtype=jnp.int32)
    onehot = segment_ids[:, :, None] == labels[None, None, :]
    return jnp.sum(jnp.where(onehot, doc_weight[:, None, :], 0), axis=2)


def adamw(grad, master, moment, second):
    moment_new = 0.9 * moment + 0.1 * grad
    second_new = 0.95 * second + 0.05 * grad * grad
    first_fix = moment_new / (1.0 - 0.9**8)
    second_fix = second_new / (1.0 - 0.95**8)
    master_new = master - 0.003 * (first_fix / (jnp.sqrt(second_fix) + 1e-08) + 0.1 * master)
    return master_new, moment_new, second_new


def reduce_path(
    inputs, gate_pre, up_pre, hidden_grad, segment_ids, doc_weight, w_gate, master, moment, second
):
    group_rows = inputs.shape[0]
    replicas = lax.axis_size("replica")
    weights = token_weights(segment_ids, doc_weight)[0]
    local_count = jnp.sum(weights)
    gate_f = gate_pre.astype(jnp.float32)
    sigmoid_gate = jax.nn.sigmoid(gate_f)
    weighted = hidden_grad.astype(jnp.float32) * weights.astype(jnp.float32)[:, None]
    gate_raw = (
        weighted * up_pre.astype(jnp.float32) * sigmoid_gate * (1.0 + gate_f * (1.0 - sigmoid_gate))
    ).astype(jnp.bfloat16)
    up_part = weighted * gate_f * sigmoid_gate
    input_part = lax.dot_general(
        gate_raw, w_gate, (((1,), (1,)), ((), ())), preferred_element_type=jnp.float32
    )
    input_summed = lax.psum_scatter(input_part, "shard", scatter_dimension=0, tiled=True)
    total = lax.psum(local_count, "replica").astype(jnp.float32)
    summed_grad = lax.psum_scatter(
        lax.dot_general(
            inputs, gate_raw, (((0,), (0,)), ((), ())), preferred_element_type=jnp.float32
        ),
        "replica",
        scatter_dimension=0,
        tiled=True,
    )
    scale = jnp.float32(group_rows * replicas) / total
    group_scale = jnp.float32(group_rows) / total
    input_grad = (input_summed * scale).astype(jnp.bfloat16)
    up_grad = (up_part * scale).astype(jnp.bfloat16)
    return (input_grad, up_grad) + adamw(summed_grad * group_scale, master, moment, second)


def flip(index, bit):
    return index + bit - 2 * bit * lax.rem(lax.div(index, bit), 2)


def exchange_kernel(
    x_hbm, gate_hbm, up_hbm, hid_hbm, seg_hbm, dw_hbm, w_hbm, ma_hbm, mo_hbm, se_hbm,
    ig_o, ug_o, gs_o, xt_o, gb, ma_o, mo_o, se_o,
    xs_v, xc_v, xg, gate_v, up_v, hid_v, seg_ref, dw_ref, w_v, xs32, xc32, xq, xp, tw_ref, gp, g32, gr, upo,
    part, rs_1, rs_2, cnt, cntr, dsum, lsem, wsem, tsem, ssem, rsem,
):
    r, s = lax.axis_index("replica"), lax.axis_index("shard")
    replicas = lax.axis_size("replica")
    core, side, across = flip(r, 1), flip(r, 2), flip(flip(r, 1), 2)
    near, mid, far = flip(s, 1), flip(s, 2), flip(s, 4)
    mid_far = flip(mid, 4)
    rows, width = gate_v.shape[0], xc_v.shape[1]
    quarter, tall = rows // QUARTERS, rows // 8
    chunk, span = gb.shape[2], part.shape[2]
    f32, bf16 = jnp.float32, jnp.bfloat16
    q = lax.rem(s, QUARTERS)

    def at_quarter(index):
        return pl.ds(pl.multiple_of(index * quarter, quarter), quarter)

    def columns(owner):
        return pl.ds(pl.multiple_of(owner * width, width), width)

    def load(src, dst, sem):
        copy = pltpu.make_async_copy(src, dst, sem)
        copy.start()
        return copy

    l_seg = load(seg_hbm, seg_ref, lsem.at[0])
    l_dw = load(dw_hbm, dw_ref, lsem.at[1])
    l_xs = load(x_hbm.at[at_quarter(q), columns(side)], xs_v.at[0], lsem.at[2])
    l_xa = load(x_hbm.at[at_quarter(q), columns(across)], xs_v.at[1], lsem.at[3])
    l_gate = load(gate_hbm, gate_v, lsem.at[4])
    l_hid = load(hid_hbm, hid_v, lsem.at[5])
    l_up = load(up_hbm, up_v, lsem.at[6])
    l_w = [
        load(w_hbm.at[pl.ds(c * span, span), :], w_v.at[pl.ds(c * span, span), :], wsem.at[c])
        for c in range(CHUNKS)
    ]
    l_xc = load(x_hbm.at[:, columns(core)], xc_v, lsem.at[7])
    l_xo = load(x_hbm.at[:, columns(r)], xg.at[pl.ds(0, rows), :], lsem.at[8])
    barrier = pltpu.get_barrier_semaphore()
    peers = [(core, s), (side, s), (across, s), (r, near), (r, mid), (r, far)]
    if "x" in KINDS:
        peers.append((r, mid_far))
    for peer in peers:
        pl.semaphore_signal(barrier, inc=1, device_id=peer, device_id_type=MESH)

    started = []

    def push(src, dst, peer):
        k = len(started)
        copy = pltpu.make_async_remote_copy(
            src_ref=src, dst_ref=dst, send_sem=ssem.at[k], recv_sem=rsem.at[k],
            device_id=peer, device_id_type=MESH,
        )
        copy.start()
        started.append(copy)
        return copy

    l_seg.wait()
    l_dw.wait()
    docs = dw_ref.shape[1]
    seg = jnp.broadcast_to(seg_ref[...].astype(f32), (128, rows)).T[:, :docs]
    labels = lax.broadcasted_iota(jnp.int32, (rows, docs), 1).astype(f32)
    dw = jnp.broadcast_to(dw_ref[...].astype(f32), (rows, docs))
    tw = jnp.sum(jnp.where(seg == labels, dw, 0.0), axis=1, keepdims=True)
    tw_ref[...] = jnp.broadcast_to(tw, tw_ref.shape)
    cnt[...] = jnp.broadcast_to(jnp.sum(tw, axis=0, keepdims=True), cnt.shape)

    l_xs.wait()
    xs32[0] = xs_v[0].astype(f32)
    l_xa.wait()
    xs32[1] = xs_v[1].astype(f32)
    pl.semaphore_wait(barrier, len(peers))
    x_first = [push(xs32.at[0], xq.at[0, 0], (side, s)), push(xs32.at[1], xq.at[1, 0], (across, s))]

    for copy in (l_gate, l_hid, l_up):
        copy.wait()
    g_side, g_core = [], []
    for k in range(CHUNKS):
        for j in range(chunk // 128):
            at, to = pl.ds(k * chunk + j * 128, 128), pl.ds(j * 128, 128)
            g = gate_v[:, at].astype(f32)
            sig = jax.nn.sigmoid(g)
            h = hid_v[:, at].astype(f32) * tw_ref[...]
            raw = (h * up_v[:, at].astype(f32) * sig * (1.0 + g * (1.0 - sig))).astype(bf16)
            upo[:, at] = h * g * sig
            gb[k, pl.ds(0, rows), to] = raw
            g32[k, :, to] = raw.astype(f32)
        g_side.append(push(g32.at[k], gr.at[1, k], (side, s)))
        if k == 0:
            counts = [push(cnt, cntr.at[n], (peer, s)) for n, peer in enumerate((core, side, across))]
        g_core.append(push(g32.at[k], gr.at[0, k], (core, s)))

    for n, position in enumerate(LAYOUT):
        block = s
        for bit in (1, 2, 4):
            if position & bit:
                block = flip(block, bit)
        at = pl.ds(pl.multiple_of(block * tall, tall), tall)
        for k in range(CHUNKS):
            gp[pl.ds(n * tall, tall), pl.ds(k * chunk, chunk)] = gb[k, at, :]

    first, second, states = {}, {}, {}

    def block(c, position):
        return part.at[c, pl.ds(LAYOUT.index(position) * tall, tall), :]

    def first_dim(c):
        return ((r, mid), 2) if KINDS[c] == "m" else ((r, near), 1)

    def second_dim(c):
        return ((r, near), 1) if KINDS[c] == "m" else ((r, mid), 2)

    def send_first(c, n):
        peer, bit = first_dim(c)
        position = bit + ((7 - bit, 3 - bit, 4, 0)[n])
        first[c, n] = push(block(c, position), rs_1.at[c, n], peer)

    def project(c):
        l_w[c].wait()
        part[c] = lax.dot_general(
            gp[...], w_v[pl.ds(c * span, span), :], (((1,), (1,)), ((), ())), preferred_element_type=f32
        )
        send_first(c, 0)

    def fetch(k):
        at = pl.ds(k * chunk, chunk)
        states[k] = [
            load(old.at[:, at], new.at[k], tsem.at[3 * k + n])
            for n, (old, new) in enumerate(((mo_hbm, mo_o), (se_hbm, se_o), (ma_hbm, ma_o)))
        ]

    def step_xc():
        l_xc.wait()
        xc32[...] = xc_v[...].astype(f32)
        x_core.append(push(xc32, xp, (core, s)))

    def forward(c, n):
        peer, bit = second_dim(c)
        kept = block(c, bit + 4 * (1 - n))
        first[c, n].wait_recv()
        kept[...] = kept[...] + rs_1[c, n]
        if KINDS[c] == "x" and n == 0:
            peer = (r, mid_far)
        second[c, n] = push(kept, rs_2.at[c, n], peer)

    def forward_far(c):
        kept = block(c, 4)
        first[c, 2].wait_recv()
        value = kept[...] + rs_1[c, 2]
        if KINDS[c] != "x":
            second[c, 0].wait_recv()
            value = value + rs_2[c, 0]
        kept[...] = value
        second[c, 2] = push(kept, rs_2.at[c, 2], (r, far))

    def finish(c):
        first[c, 3].wait_recv()
        total = block(c, 0)[...] + rs_1[c, 3]
        for n in (0, 1, 2) if KINDS[c] == "x" else (1, 2):
            second[c, n].wait_recv()
            total = total + rs_2[c, n]
        ig_o[:, pl.ds(c * span, span)] = (total * scale[0]).astype(bf16)

    def keep_x(group, slot, index):
        to = pl.ds(pl.multiple_of((group + 2) * rows + index * quarter, quarter), quarter)
        xg[to, :] = xq[group, slot].astype(bf16)

    def turn(group):
        xt_o[:, pl.ds(group * rows, rows)] = xg[pl.ds(group * rows, rows), :].T

    def step_x(group):
        x_first[group].wait_recv()
        x_near[group] = push(xq.at[group, 0], xq.at[group, 1], (r, near))
        x_mid[group] = push(xq.at[group, 0], xq.at[group, 2], (r, mid))
        keep_x(group, 0, q)

    def step_x_last(group):
        if X_LAST[group] == "mid":
            x_near[group].wait_recv()
            x_last[group] = push(xq.at[group, 1], xq.at[group, 3], (r, mid))
        else:
            x_mid[group].wait_recv()
            x_last[group] = push(xq.at[group, 2], xq.at[group, 3], (r, near))

    def step_x_end(group):
        if X_LAST[group] == "mid":
            x_mid[group].wait_recv()
        else:
            x_near[group].wait_recv()
        x_last[group].wait_recv()
        keep_x(group, 1, lax.rem(near, QUARTERS))
        keep_x(group, 2, lax.rem(mid, QUARTERS))
        keep_x(group, 3, lax.rem(flip(near, 2), QUARTERS))
        turn(group + 2)

    def step_own():
        l_xo.wait()
        turn(0)
        x_core[0].wait_recv()
        xg[pl.ds(rows, rows), :] = xp[...].astype(bf16)
        turn(1)

    def store_g(k, group):
        value = gr[group, k].astype(bf16)
        gb[k, pl.ds((group + 1) * rows, rows), :] = value

    def step_core():
        for k in range(CHUNKS):
            g_core[k].wait_recv()
            store_g(k, 0)

    def relay(k):
        g_side[k].wait_recv()
        g_across[k] = push(gr.at[1, k], gr.at[2, k], (core, s))
        store_g(k, 1)

    def step_scale():
        for copy in counts:
            copy.wait_recv()
        total = (cnt[...] + cntr[0] + cntr[1] + cntr[2])[0:1, 0:1]
        scale.append(f32(rows * replicas) / total)
        scale.append(f32(rows) / total)
        gs_o[...] = jnp.broadcast_to(scale[1], gs_o.shape)
        ug_o[...] = (upo[...] * scale[0]).astype(bf16)

    def take(k):
        g_across[k].wait_recv()
        store_g(k, 2)

    def optimize(k):
        dsum[...] = jnp.dot(xt_o[...], gb[k], preferred_element_type=f32)
        for copy in states[k]:
            copy.wait()
        for n in range(width // BAND):
            at = pl.ds(n * BAND, BAND)
            update(dsum[at, :] * scale[1], ma_o.at[k, at], mo_o.at[k, at], se_o.at[k, at],
                   ma_o.at[k, at], mo_o.at[k, at], se_o.at[k, at])

    x_core, x_near, x_mid, x_last, g_across, scale = [], {}, {}, {}, {}, []
    steps = {
        "xc": step_xc, "own": step_own, "core": step_core, "scale": step_scale, "x": step_x, "xl": step_x_last,
        "xe": step_x_end, "st": fetch, "p": project,
        "b": lambda c: send_first(c, 1), "c": lambda c: send_first(c, 2), "d": lambda c: send_first(c, 3),
        "a": lambda c: forward(c, 0), "e": lambda c: forward(c, 1), "f": forward_far, "i": finish, "g": relay, "t": take, "opt": optimize,
    }
    for name in ORDER:
        kind = name.rstrip("0123456789")
        index = name[len(kind):]
        steps[kind](*([int(index)] if index else []))
    for k in range(DONE, CHUNKS):
        for copy in states[k]:
            copy.wait()
    for copy in started:
        copy.wait_send()


def update(grad, ma, mo, se, ma_to, mo_to, se_to):
    moment_new = 0.9 * mo[...] + 0.1 * grad
    second_new = 0.95 * se[...] + 0.05 * grad * grad
    master = ma[...]
    mo_to[...] = moment_new
    se_to[...] = second_new
    first_fix = moment_new * (1.0 / (1.0 - 0.9**8))
    second_fix = second_new * (1.0 / (1.0 - 0.95**8))
    ma_to[...] = master - 0.003 * (first_fix / (jnp.sqrt(second_fix) + 1e-08) + 0.1 * master)


def exchange(inputs, gate_pre, up_pre, hidden_grad, segment_ids, doc_weight, w_gate, master, moment, second):
    replicas, shards = lax.axis_size("replica"), lax.axis_size("shard")
    rows, features = inputs.shape
    hidden = gate_pre.shape[1]
    width, tall, quarter = features // replicas, rows // shards, rows // QUARTERS
    chunk, span = hidden // CHUNKS, features // CHUNKS
    f32, bf16 = jnp.float32, jnp.bfloat16
    hbm = pl.BlockSpec(memory_space=pltpu.HBM)
    vmem = pl.BlockSpec(memory_space=pltpu.VMEM)
    copies = 2 + 3 + 2 * CHUNKS + 1 + 6 + CHUNKS + 7 * CHUNKS
    state = pltpu.VMEM((CHUNKS, width, chunk), f32)
    operands = (inputs, gate_pre, up_pre, hidden_grad, segment_ids, doc_weight, w_gate, master, moment, second)
    return pl.pallas_call(
        exchange_kernel,
        out_shape=(
            pltpu.VMEM((tall, features), bf16),
            pltpu.VMEM((rows, hidden), bf16),
            pltpu.VMEM((8, chunk), f32),
            pltpu.VMEM((width, replicas * rows), bf16),
            pltpu.VMEM((CHUNKS, replicas * rows, chunk), bf16),
            state,
            state,
            state,
        ),
        in_specs=[hbm] * 10,
        out_specs=(vmem,) * 8,
        scratch_shapes=[
            pltpu.VMEM((2, quarter, width), bf16),
            pltpu.VMEM((rows, width), bf16),
            pltpu.VMEM((replicas * rows, width), bf16),
            pltpu.VMEM((rows, hidden), bf16),
            pltpu.VMEM((rows, hidden), bf16),
            pltpu.VMEM((rows, hidden), bf16),
            pltpu.VMEM(segment_ids.shape, jnp.int32),
            pltpu.VMEM(doc_weight.shape, jnp.int32),
            pltpu.VMEM((features, hidden), bf16),
            pltpu.VMEM((2, quarter, width), f32),
            pltpu.VMEM((rows, width), f32),
            pltpu.VMEM((2, QUARTERS, quarter, width), f32),
            pltpu.VMEM((rows, width), f32),
            pltpu.VMEM((rows, 128), f32),
            pltpu.VMEM((rows, hidden), bf16),
            pltpu.VMEM((CHUNKS, rows, chunk), f32),
            pltpu.VMEM((3, CHUNKS, rows, chunk), f32),
            pltpu.VMEM((rows, hidden), f32),
            pltpu.VMEM((CHUNKS, rows, span), f32),
            pltpu.VMEM((CHUNKS, 4, tall, span), f32),
            pltpu.VMEM((CHUNKS, 3, tall, span), f32),
            pltpu.VMEM((8, 128), f32),
            pltpu.VMEM((3, 8, 128), f32),
            pltpu.VMEM((width, chunk), f32),
            pltpu.SemaphoreType.DMA((9,)),
            pltpu.SemaphoreType.DMA((CHUNKS,)),
            pltpu.SemaphoreType.DMA((3 * CHUNKS,)),
            pltpu.SemaphoreType.DMA((copies,)),
            pltpu.SemaphoreType.DMA((copies,)),
        ],
        compiler_params=pltpu.CompilerParams(
            collective_id=0, has_side_effects=True, vmem_limit_bytes=40 * 1024 * 1024
        ),
        cost_estimate=pl.CostEstimate(
            flops=4 * rows * hidden * features, bytes_accessed=12 * 1024 * 1024, transcendentals=0
        ),
        name="exchange",
    )(*[pltpu.with_memory_space_constraint(operand, pltpu.HBM) for operand in operands])


def step_kernel(
    ig_ref, ug_ref, gs_ref, xt_ref, gb_ref, ma_ref, mo_ref, se_ref,
    ig_hbm, ug_hbm, ma_hbm, mo_hbm, se_hbm,
    ma_v, mo_v, se_v, sems,
):
    written = []
    chunks, width, chunk = ma_ref.shape

    def write(src, dst):
        copy = pltpu.make_async_copy(src, dst, sems.at[len(written)])
        copy.start()
        written.append(copy)

    for k in range(DONE):
        for src, dst in ((mo_ref, mo_hbm), (se_ref, se_hbm), (ma_ref, ma_hbm)):
            write(src.at[k], dst.at[:, pl.ds(k * chunk, chunk)])
    write(ig_ref, ig_hbm)
    write(ug_ref, ug_hbm)
    group_scale = gs_ref[0:1, :]
    half = width // 2
    for k in range(DONE, chunks):
        for m in range(2):
            rows = pl.ds(m * half, half)
            raw = jnp.dot(xt_ref[rows, :], gb_ref[k], preferred_element_type=jnp.float32)
            mo_v[k - DONE, rows, :] = raw * group_scale
            for n in range(half // BAND):
                at = pl.ds(m * half + n * BAND, BAND)
                update(mo_v[k - DONE, at, :], ma_ref.at[k, at], mo_ref.at[k, at], se_ref.at[k, at],
                       ma_v.at[k - DONE, at], mo_v.at[k - DONE, at], se_v.at[k - DONE, at])
            for src, dst in ((mo_v, mo_hbm), (se_v, se_hbm), (ma_v, ma_hbm)):
                write(src.at[k - DONE, rows], dst.at[rows, pl.ds(k * chunk, chunk)])
    for copy in written:
        copy.wait()


def step(ig, ug, gs, xt, gb, ma, mo, se):
    chunks, width, chunk = ma.shape
    f32 = jnp.float32
    hbm = pl.BlockSpec(memory_space=pltpu.HBM)
    vmem = pl.BlockSpec(memory_space=pltpu.VMEM)
    late = pltpu.VMEM((chunks - DONE, width, chunk), f32)
    return pl.pallas_call(
        step_kernel,
        out_shape=(
            jax.ShapeDtypeStruct(ig.shape, ig.dtype),
            jax.ShapeDtypeStruct(ug.shape, ug.dtype),
        )
        + (jax.ShapeDtypeStruct((width, chunks * chunk), f32),) * 3,
        in_specs=[vmem] * 8,
        out_specs=(hbm,) * 5,
        scratch_shapes=[late, late, late, pltpu.SemaphoreType.DMA((2 + 3 * DONE + 6 * (chunks - DONE),))],
        compiler_params=pltpu.CompilerParams(vmem_limit_bytes=40 * 1024 * 1024),
        name="step",
    )(ig, ug, gs, xt, gb, ma, mo, se)


def gather_path(*args):
    return step(*exchange(*args))


def on_device(*args):
    inputs, gate_pre = args[:2]
    replicas, shards = lax.axis_size("replica"), lax.axis_size("shard")
    rows, features = inputs.shape
    hidden = gate_pre.shape[1]
    gathered = replicas * rows * (features // replicas + hidden)
    fits = rows % (QUARTERS * 32) == 0 and features % (replicas * 128) == 0 and hidden % (CHUNKS * 128) == 0
    if (replicas, shards) == (4, 8) and fits and gathered <= features * hidden:
        return gather_path(*args)
    return reduce_path(*args)


def solution(mesh):
    in_specs = (
        P("replica", None),
        P("replica", "shard"),
        P("replica", "shard"),
        P("replica", "shard"),
        P("replica", None),
        P("replica", None),
        P(None, "shard"),
        P("replica", "shard"),
        P("replica", "shard"),
        P("replica", "shard"),
    )
    out_specs = (
        P(("replica", "shard"), None),
        P("replica", "shard"),
        P("replica", "shard"),
        P("replica", "shard"),
        P("replica", "shard"),
    )
    return jax.shard_map(
        on_device, mesh=mesh, in_specs=in_specs, out_specs=out_specs, check_vma=False
    )
```

```python
import functools

import jax
import jax.numpy as jnp
from jax import lax
from jax.experimental import pallas as pl
from jax.experimental.pallas import tpu as pltpu
from jax.sharding import PartitionSpec as P

MESH = pl.DeviceIdType.MESH
QUARTERS = 4
CHUNKS = 4
BAND = 64
LAYOUT = (7, 3, 5, 1, 6, 2, 4, 0)
KINDS = "mhmh"
X_LAST = ("near", "near")
DONE = 3
ORDER = (
    "p2", "p1", "c1", "b2", "p0", "b1", "b0", "p3", "st0", "st1", "st2", "st3", "xc", "c0", "b3",
    "x1", "a2", "c2", "a1", "x0", "a3", "c3", "a0", "e3", "g0", "d0", "f1", "xl1", "own", "xl0",
    "f2", "d2", "e1", "t0", "f0", "e0", "f3", "g1", "core", "xe1", "scale", "d1", "d3", "e2", "t1",
    "g2", "xe0", "opt0", "opt1", "t2", "g3", "opt2", "i0", "i2", "i1", "i3", "t3",
)


def token_weights(segment_ids, doc_weight):
    labels = jnp.arange(doc_weight.shape[1], dtype=jnp.int32)
    onehot = segment_ids[:, :, None] == labels[None, None, :]
    return jnp.sum(jnp.where(onehot, doc_weight[:, None, :], 0), axis=2)


def adamw(grad, master, moment, second):
    moment_new = 0.9 * moment + 0.1 * grad
    second_new = 0.95 * second + 0.05 * grad * grad
    first_fix = moment_new / (1.0 - 0.9**8)
    second_fix = second_new / (1.0 - 0.95**8)
    master_new = master - 0.003 * (first_fix / (jnp.sqrt(second_fix) + 1e-08) + 0.1 * master)
    return master_new, moment_new, second_new


def reduce_path(
    inputs, gate_pre, up_pre, hidden_grad, segment_ids, doc_weight, w_gate, master, moment, second
):
    group_rows = inputs.shape[0]
    replicas = lax.axis_size("replica")
    weights = token_weights(segment_ids, doc_weight)[0]
    local_count = jnp.sum(weights)
    gate_f = gate_pre.astype(jnp.float32)
    sigmoid_gate = jax.nn.sigmoid(gate_f)
    weighted = hidden_grad.astype(jnp.float32) * weights.astype(jnp.float32)[:, None]
    gate_raw = (
        weighted * up_pre.astype(jnp.float32) * sigmoid_gate * (1.0 + gate_f * (1.0 - sigmoid_gate))
    ).astype(jnp.bfloat16)
    up_part = weighted * gate_f * sigmoid_gate
    input_part = lax.dot_general(
        gate_raw, w_gate, (((1,), (1,)), ((), ())), preferred_element_type=jnp.float32
    )
    input_summed = lax.psum_scatter(input_part, "shard", scatter_dimension=0, tiled=True)
    total = lax.psum(local_count, "replica").astype(jnp.float32)
    summed_grad = lax.psum_scatter(
        lax.dot_general(
            inputs, gate_raw, (((0,), (0,)), ((), ())), preferred_element_type=jnp.float32
        ),
        "replica",
        scatter_dimension=0,
        tiled=True,
    )
    scale = jnp.float32(group_rows * replicas) / total
    group_scale = jnp.float32(group_rows) / total
    input_grad = (input_summed * scale).astype(jnp.bfloat16)
    up_grad = (up_part * scale).astype(jnp.bfloat16)
    return (input_grad, up_grad) + adamw(summed_grad * group_scale, master, moment, second)


def flip(index, bit):
    return index + bit - 2 * bit * lax.rem(lax.div(index, bit), 2)


def exchange_kernel(
    x_hbm, gate_hbm, up_hbm, hid_hbm, seg_hbm, dw_hbm, w_hbm, ma_hbm, mo_hbm, se_hbm,
    ig_o, ug_o, gs_o, xt_o, gb, ma_o, mo_o, se_o,
    xs_v, xc_v, xg, gate_v, up_v, hid_v, seg_ref, dw_ref, w_v, xs32, xc32, xq, xp, tw_ref, gp, g32, gr, upo,
    part, rs_1, rs_2, cnt, cntr, dsum, lsem, wsem, tsem, ssem, rsem,
):
    r, s = lax.axis_index("replica"), lax.axis_index("shard")
    replicas = lax.axis_size("replica")
    core, side, across = flip(r, 1), flip(r, 2), flip(flip(r, 1), 2)
    near, mid, far = flip(s, 1), flip(s, 2), flip(s, 4)
    mid_far = flip(mid, 4)
    rows, width = gate_v.shape[0], xc_v.shape[1]
    quarter, tall = rows // QUARTERS, rows // 8
    chunk, span = gb.shape[2], part.shape[2]
    f32, bf16 = jnp.float32, jnp.bfloat16
    q = lax.rem(s, QUARTERS)

    def at_quarter(index):
        return pl.ds(pl.multiple_of(index * quarter, quarter), quarter)

    def columns(owner):
        return pl.ds(pl.multiple_of(owner * width, width), width)

    def load(src, dst, sem):
        copy = pltpu.make_async_copy(src, dst, sem)
        copy.start()
        return copy

    barrier = pltpu.get_barrier_semaphore()
    peers = [(core, s), (side, s), (across, s), (r, near), (r, mid), (r, far)]
    if "x" in KINDS:
        peers.append((r, mid_far))
    for peer in peers:
        pl.semaphore_signal(barrier, inc=1, device_id=peer, device_id_type=MESH)

    l_seg = load(seg_hbm, seg_ref, lsem.at[0])
    l_dw = load(dw_hbm, dw_ref, lsem.at[1])
    l_xs = load(x_hbm.at[at_quarter(q), columns(side)], xs_v.at[0], lsem.at[2])
    l_xa = load(x_hbm.at[at_quarter(q), columns(across)], xs_v.at[1], lsem.at[3])
    l_gate = load(gate_hbm, gate_v, lsem.at[4])
    l_hid = load(hid_hbm, hid_v, lsem.at[5])
    l_up = load(up_hbm, up_v, lsem.at[6])
    l_w = [
        load(w_hbm.at[pl.ds(c * span, span), :], w_v.at[pl.ds(c * span, span), :], wsem.at[c])
        for c in range(CHUNKS)
    ]
    l_xc = load(x_hbm.at[:, columns(core)], xc_v, lsem.at[7])
    l_xo = load(x_hbm.at[:, columns(r)], xg.at[pl.ds(0, rows), :], lsem.at[8])
    started = []

    def push(src, dst, peer):
        k = len(started)
        copy = pltpu.make_async_remote_copy(
            src_ref=src, dst_ref=dst, send_sem=ssem.at[k], recv_sem=rsem.at[k],
            device_id=peer, device_id_type=MESH,
        )
        copy.start()
        started.append(copy)
        return copy

    l_seg.wait()
    l_dw.wait()
    docs = dw_ref.shape[1]
    seg = jnp.broadcast_to(seg_ref[...].astype(f32), (128, rows)).T[:, :docs]
    labels = lax.broadcasted_iota(jnp.int32, (rows, docs), 1).astype(f32)
    dw = jnp.broadcast_to(dw_ref[...].astype(f32), (rows, docs))
    tw = jnp.sum(jnp.where(seg == labels, dw, 0.0), axis=1, keepdims=True)
    tw_ref[...] = jnp.broadcast_to(tw, tw_ref.shape)
    cnt[...] = jnp.broadcast_to(jnp.sum(tw, axis=0, keepdims=True), cnt.shape)

    l_xs.wait()
    xs32[0] = xs_v[0].astype(f32)
    l_xa.wait()
    xs32[1] = xs_v[1].astype(f32)
    pl.semaphore_wait(barrier, len(peers))
    counts = [push(cnt, cntr.at[n], (peer, s)) for n, peer in enumerate((core, side, across))]
    x_first = [push(xs32.at[0], xq.at[0, 0], (side, s)), push(xs32.at[1], xq.at[1, 0], (across, s))]

    for copy in (l_gate, l_hid, l_up):
        copy.wait()
    g_side, g_core = [], []
    for k in range(CHUNKS):
        for j in range(chunk // 128):
            at, to = pl.ds(k * chunk + j * 128, 128), pl.ds(j * 128, 128)
            g = gate_v[:, at].astype(f32)
            sig = jax.nn.sigmoid(g)
            h = hid_v[:, at].astype(f32) * tw_ref[...]
            raw = (h * up_v[:, at].astype(f32) * sig * (1.0 + g * (1.0 - sig))).astype(bf16)
            upo[:, at] = h * g * sig
            gb[k, pl.ds(0, rows), to] = raw
            g32[k, :, to] = raw.astype(f32)
        g_side.append(push(g32.at[k], gr.at[1, k], (side, s)))
        g_core.append(push(g32.at[k], gr.at[0, k], (core, s)))

    for n, position in enumerate(LAYOUT):
        block = s
        for bit in (1, 2, 4):
            if position & bit:
                block = flip(block, bit)
        at = pl.ds(pl.multiple_of(block * tall, tall), tall)
        for k in range(CHUNKS):
            gp[pl.ds(n * tall, tall), pl.ds(k * chunk, chunk)] = gb[k, at, :]

    first, second, states = {}, {}, {}

    def block(c, position):
        return part.at[c, pl.ds(LAYOUT.index(position) * tall, tall), :]

    def first_dim(c):
        return ((r, mid), 2) if KINDS[c] == "m" else ((r, near), 1)

    def second_dim(c):
        return ((r, near), 1) if KINDS[c] == "m" else ((r, mid), 2)

    def send_first(c, n):
        peer, bit = first_dim(c)
        position = bit + ((7 - bit, 3 - bit, 4, 0)[n])
        first[c, n] = push(block(c, position), rs_1.at[c, n], peer)

    def project(c):
        l_w[c].wait()
        part[c] = lax.dot_general(
            gp[...], w_v[pl.ds(c * span, span), :], (((1,), (1,)), ((), ())), preferred_element_type=f32
        )
        send_first(c, 0)

    def fetch(k):
        at = pl.ds(k * chunk, chunk)
        states[k] = [
            load(old.at[:, at], new.at[k], tsem.at[3 * k + n])
            for n, (old, new) in enumerate(((mo_hbm, mo_o), (se_hbm, se_o), (ma_hbm, ma_o)))
        ]

    def step_xc():
        l_xc.wait()
        xc32[...] = xc_v[...].astype(f32)
        x_core.append(push(xc32, xp, (core, s)))

    def forward(c, n):
        peer, bit = second_dim(c)
        kept = block(c, bit + 4 * (1 - n))
        first[c, n].wait_recv()
        kept[...] = kept[...] + rs_1[c, n]
        if KINDS[c] == "x" and n == 0:
            peer = (r, mid_far)
        second[c, n] = push(kept, rs_2.at[c, n], peer)

    def forward_far(c):
        kept = block(c, 4)
        first[c, 2].wait_recv()
        value = kept[...] + rs_1[c, 2]
        if KINDS[c] != "x":
            second[c, 0].wait_recv()
            value = value + rs_2[c, 0]
        kept[...] = value
        second[c, 2] = push(kept, rs_2.at[c, 2], (r, far))

    def finish(c):
        first[c, 3].wait_recv()
        total = block(c, 0)[...] + rs_1[c, 3]
        for n in (0, 1, 2) if KINDS[c] == "x" else (1, 2):
            second[c, n].wait_recv()
            total = total + rs_2[c, n]
        ig_o[:, pl.ds(c * span, span)] = (total * scale[0]).astype(bf16)

    def keep_x(group, slot, index):
        to = pl.ds(pl.multiple_of((group + 2) * rows + index * quarter, quarter), quarter)
        xg[to, :] = xq[group, slot].astype(bf16)

    def turn(group):
        xt_o[:, pl.ds(group * rows, rows)] = xg[pl.ds(group * rows, rows), :].T

    def step_x(group):
        x_first[group].wait_recv()
        x_near[group] = push(xq.at[group, 0], xq.at[group, 1], (r, near))
        x_mid[group] = push(xq.at[group, 0], xq.at[group, 2], (r, mid))
        keep_x(group, 0, q)

    def step_x_last(group):
        if X_LAST[group] == "mid":
            x_near[group].wait_recv()
            x_last[group] = push(xq.at[group, 1], xq.at[group, 3], (r, mid))
        else:
            x_mid[group].wait_recv()
            x_last[group] = push(xq.at[group, 2], xq.at[group, 3], (r, near))

    def step_x_end(group):
        if X_LAST[group] == "mid":
            x_mid[group].wait_recv()
        else:
            x_near[group].wait_recv()
        x_last[group].wait_recv()
        keep_x(group, 1, lax.rem(near, QUARTERS))
        keep_x(group, 2, lax.rem(mid, QUARTERS))
        keep_x(group, 3, lax.rem(flip(near, 2), QUARTERS))
        turn(group + 2)

    def step_own():
        l_xo.wait()
        turn(0)
        x_core[0].wait_recv()
        xg[pl.ds(rows, rows), :] = xp[...].astype(bf16)
        turn(1)

    def store_g(k, group):
        value = gr[group, k].astype(bf16)
        gb[k, pl.ds((group + 1) * rows, rows), :] = value

    def step_core():
        for k in range(CHUNKS):
            g_core[k].wait_recv()
            store_g(k, 0)

    def relay(k):
        g_side[k].wait_recv()
        g_across[k] = push(gr.at[1, k], gr.at[2, k], (core, s))
        store_g(k, 1)

    def step_scale():
        for copy in counts:
            copy.wait_recv()
        total = (cnt[...] + cntr[0] + cntr[1] + cntr[2])[0:1, 0:1]
        scale.append(f32(rows * replicas) / total)
        scale.append(f32(rows) / total)
        gs_o[...] = jnp.broadcast_to(scale[1], gs_o.shape)
        ug_o[...] = (upo[...] * scale[0]).astype(bf16)

    def take(k):
        g_across[k].wait_recv()
        store_g(k, 2)

    def optimize(k):
        dsum[...] = jnp.dot(xt_o[...], gb[k], preferred_element_type=f32)
        for copy in states[k]:
            copy.wait()
        for n in range(width // BAND):
            at = pl.ds(n * BAND, BAND)
            update(dsum[at, :] * scale[1], ma_o.at[k, at], mo_o.at[k, at], se_o.at[k, at],
                   ma_o.at[k, at], mo_o.at[k, at], se_o.at[k, at])

    x_core, x_near, x_mid, x_last, g_across, scale = [], {}, {}, {}, {}, []
    steps = {
        "xc": step_xc, "own": step_own, "core": step_core, "scale": step_scale, "x": step_x, "xl": step_x_last,
        "xe": step_x_end, "st": fetch, "p": project,
        "b": lambda c: send_first(c, 1), "c": lambda c: send_first(c, 2), "d": lambda c: send_first(c, 3),
        "a": lambda c: forward(c, 0), "e": lambda c: forward(c, 1), "f": forward_far, "i": finish, "g": relay, "t": take, "opt": optimize,
    }
    for name in ORDER:
        kind = name.rstrip("0123456789")
        index = name[len(kind):]
        steps[kind](*([int(index)] if index else []))
    for k in range(DONE, CHUNKS):
        for copy in states[k]:
            copy.wait()
    for copy in started:
        copy.wait_send()


def update(grad, ma, mo, se, ma_to, mo_to, se_to):
    moment_new = 0.9 * mo[...] + 0.1 * grad
    second_new = 0.95 * se[...] + 0.05 * grad * grad
    master = ma[...]
    mo_to[...] = moment_new
    se_to[...] = second_new
    first_fix = moment_new * (1.0 / (1.0 - 0.9**8))
    second_fix = second_new * (1.0 / (1.0 - 0.95**8))
    ma_to[...] = master - 0.003 * (first_fix / (jnp.sqrt(second_fix) + 1e-08) + 0.1 * master)


def exchange(inputs, gate_pre, up_pre, hidden_grad, segment_ids, doc_weight, w_gate, master, moment, second):
    replicas, shards = lax.axis_size("replica"), lax.axis_size("shard")
    rows, features = inputs.shape
    hidden = gate_pre.shape[1]
    width, tall, quarter = features // replicas, rows // shards, rows // QUARTERS
    chunk, span = hidden // CHUNKS, features // CHUNKS
    f32, bf16 = jnp.float32, jnp.bfloat16
    hbm = pl.BlockSpec(memory_space=pltpu.HBM)
    vmem = pl.BlockSpec(memory_space=pltpu.VMEM)
    copies = 2 + 3 + 2 * CHUNKS + 1 + 6 + CHUNKS + 7 * CHUNKS
    state = pltpu.VMEM((CHUNKS, width, chunk), f32)
    operands = (inputs, gate_pre, up_pre, hidden_grad, segment_ids, doc_weight, w_gate, master, moment, second)
    return pl.pallas_call(
        exchange_kernel,
        out_shape=(
            pltpu.VMEM((tall, features), bf16),
            pltpu.VMEM((rows, hidden), bf16),
            pltpu.VMEM((8, chunk), f32),
            pltpu.VMEM((width, replicas * rows), bf16),
            pltpu.VMEM((CHUNKS, replicas * rows, chunk), bf16),
            state,
            state,
            state,
        ),
        in_specs=[hbm] * 10,
        out_specs=(vmem,) * 8,
        scratch_shapes=[
            pltpu.VMEM((2, quarter, width), bf16),
            pltpu.VMEM((rows, width), bf16),
            pltpu.VMEM((replicas * rows, width), bf16),
            pltpu.VMEM((rows, hidden), bf16),
            pltpu.VMEM((rows, hidden), bf16),
            pltpu.VMEM((rows, hidden), bf16),
            pltpu.VMEM(segment_ids.shape, jnp.int32),
            pltpu.VMEM(doc_weight.shape, jnp.int32),
            pltpu.VMEM((features, hidden), bf16),
            pltpu.VMEM((2, quarter, width), f32),
            pltpu.VMEM((rows, width), f32),
            pltpu.VMEM((2, QUARTERS, quarter, width), f32),
            pltpu.VMEM((rows, width), f32),
            pltpu.VMEM((rows, 128), f32),
            pltpu.VMEM((rows, hidden), bf16),
            pltpu.VMEM((CHUNKS, rows, chunk), f32),
            pltpu.VMEM((3, CHUNKS, rows, chunk), f32),
            pltpu.VMEM((rows, hidden), f32),
            pltpu.VMEM((CHUNKS, rows, span), f32),
            pltpu.VMEM((CHUNKS, 4, tall, span), f32),
            pltpu.VMEM((CHUNKS, 3, tall, span), f32),
            pltpu.VMEM((8, 128), f32),
            pltpu.VMEM((3, 8, 128), f32),
            pltpu.VMEM((width, chunk), f32),
            pltpu.SemaphoreType.DMA((9,)),
            pltpu.SemaphoreType.DMA((CHUNKS,)),
            pltpu.SemaphoreType.DMA((3 * CHUNKS,)),
            pltpu.SemaphoreType.DMA((copies,)),
            pltpu.SemaphoreType.DMA((copies,)),
        ],
        compiler_params=pltpu.CompilerParams(
            collective_id=0, has_side_effects=True, vmem_limit_bytes=40 * 1024 * 1024
        ),
        cost_estimate=pl.CostEstimate(
            flops=4 * rows * hidden * features, bytes_accessed=12 * 1024 * 1024, transcendentals=0
        ),
        name="exchange",
    )(*[pltpu.with_memory_space_constraint(operand, pltpu.HBM) for operand in operands])


def step_kernel(
    ig_ref, ug_ref, gs_ref, xt_ref, gb_ref, ma_ref, mo_ref, se_ref,
    ig_hbm, ug_hbm, ma_hbm, mo_hbm, se_hbm,
    ma_v, mo_v, se_v, sems,
):
    written = []
    chunks, width, chunk = ma_ref.shape

    def write(src, dst):
        copy = pltpu.make_async_copy(src, dst, sems.at[len(written)])
        copy.start()
        written.append(copy)

    for k in range(DONE):
        for src, dst in ((mo_ref, mo_hbm), (se_ref, se_hbm), (ma_ref, ma_hbm)):
            write(src.at[k], dst.at[:, pl.ds(k * chunk, chunk)])
    write(ig_ref, ig_hbm)
    write(ug_ref, ug_hbm)
    group_scale = gs_ref[0:1, :]
    half = width // 2
    for k in range(DONE, chunks):
        for m in range(2):
            rows = pl.ds(m * half, half)
            raw = jnp.dot(xt_ref[rows, :], gb_ref[k], preferred_element_type=jnp.float32)
            mo_v[k - DONE, rows, :] = raw * group_scale
            for n in range(half // BAND):
                at = pl.ds(m * half + n * BAND, BAND)
                update(mo_v[k - DONE, at, :], ma_ref.at[k, at], mo_ref.at[k, at], se_ref.at[k, at],
                       ma_v.at[k - DONE, at], mo_v.at[k - DONE, at], se_v.at[k - DONE, at])
            for src, dst in ((mo_v, mo_hbm), (se_v, se_hbm), (ma_v, ma_hbm)):
                write(src.at[k - DONE, rows], dst.at[rows, pl.ds(k * chunk, chunk)])
    for copy in written:
        copy.wait()


def step(ig, ug, gs, xt, gb, ma, mo, se):
    chunks, width, chunk = ma.shape
    f32 = jnp.float32
    hbm = pl.BlockSpec(memory_space=pltpu.HBM)
    vmem = pl.BlockSpec(memory_space=pltpu.VMEM)
    late = pltpu.VMEM((chunks - DONE, width, chunk), f32)
    return pl.pallas_call(
        step_kernel,
        out_shape=(
            jax.ShapeDtypeStruct(ig.shape, ig.dtype),
            jax.ShapeDtypeStruct(ug.shape, ug.dtype),
        )
        + (jax.ShapeDtypeStruct((width, chunks * chunk), f32),) * 3,
        in_specs=[vmem] * 8,
        out_specs=(hbm,) * 5,
        scratch_shapes=[late, late, late, pltpu.SemaphoreType.DMA((2 + 3 * DONE + 6 * (chunks - DONE),))],
        compiler_params=pltpu.CompilerParams(vmem_limit_bytes=40 * 1024 * 1024),
        name="step",
    )(ig, ug, gs, xt, gb, ma, mo, se)


def gather_path(*args):
    return step(*exchange(*args))


def on_device(*args):
    inputs, gate_pre = args[:2]
    replicas, shards = lax.axis_size("replica"), lax.axis_size("shard")
    rows, features = inputs.shape
    hidden = gate_pre.shape[1]
    gathered = replicas * rows * (features // replicas + hidden)
    fits = rows % (QUARTERS * 32) == 0 and features % (replicas * 128) == 0 and hidden % (CHUNKS * 128) == 0
    if (replicas, shards) == (4, 8) and fits and gathered <= features * hidden:
        return gather_path(*args)
    return reduce_path(*args)


def solution(mesh):
    in_specs = (
        P("replica", None),
        P("replica", "shard"),
        P("replica", "shard"),
        P("replica", "shard"),
        P("replica", None),
        P("replica", None),
        P(None, "shard"),
        P("replica", "shard"),
        P("replica", "shard"),
        P("replica", "shard"),
    )
    out_specs = (
        P(("replica", "shard"), None),
        P("replica", "shard"),
        P("replica", "shard"),
        P("replica", "shard"),
        P("replica", "shard"),
    )
    return jax.shard_map(
        on_device, mesh=mesh, in_specs=in_specs, out_specs=out_specs, check_vma=False
    )
```

```python
import functools

import jax
import jax.numpy as jnp
from jax import lax
from jax.experimental import pallas as pl
from jax.experimental.pallas import tpu as pltpu
from jax.sharding import PartitionSpec as P

MESH = pl.DeviceIdType.MESH
QUARTERS = 4
CHUNKS = 4
BAND = 64
LAYOUT = (7, 3, 5, 1, 6, 2, 4, 0)
KINDS = "mhmh"
X_LAST = ("near", "near")
DONE = 3
ORDER = (
    "p0", "p1", "c1", "d0", "b1", "c0", "xc", "p3", "p2", "tell", "st0", "st1", "st2", "st3", "b0",
    "core", "x1", "a0", "c3", "a1", "x0", "e1", "a2", "c2", "a3", "far", "f0", "b3", "f1", "b2",
    "xl1", "g0", "own", "xl0", "g1", "e0", "t1", "e3", "f3", "scale", "d1", "d3", "d2", "f2", "e2",
    "g2", "xe1", "xe0", "t0", "opt0", "i0", "g3", "opt1", "t2", "i1", "opt2", "t3", "i3", "i2",
)
LATE = 0


def token_weights(segment_ids, doc_weight):
    labels = jnp.arange(doc_weight.shape[1], dtype=jnp.int32)
    onehot = segment_ids[:, :, None] == labels[None, None, :]
    return jnp.sum(jnp.where(onehot, doc_weight[:, None, :], 0), axis=2)


def adamw(grad, master, moment, second):
    moment_new = 0.9 * moment + 0.1 * grad
    second_new = 0.95 * second + 0.05 * grad * grad
    first_fix = moment_new / (1.0 - 0.9**8)
    second_fix = second_new / (1.0 - 0.95**8)
    master_new = master - 0.003 * (first_fix / (jnp.sqrt(second_fix) + 1e-08) + 0.1 * master)
    return master_new, moment_new, second_new


def reduce_path(
    inputs, gate_pre, up_pre, hidden_grad, segment_ids, doc_weight, w_gate, master, moment, second
):
    group_rows = inputs.shape[0]
    replicas = lax.axis_size("replica")
    weights = token_weights(segment_ids, doc_weight)[0]
    local_count = jnp.sum(weights)
    gate_f = gate_pre.astype(jnp.float32)
    sigmoid_gate = jax.nn.sigmoid(gate_f)
    weighted = hidden_grad.astype(jnp.float32) * weights.astype(jnp.float32)[:, None]
    gate_raw = (
        weighted * up_pre.astype(jnp.float32) * sigmoid_gate * (1.0 + gate_f * (1.0 - sigmoid_gate))
    ).astype(jnp.bfloat16)
    up_part = weighted * gate_f * sigmoid_gate
    input_part = lax.dot_general(
        gate_raw, w_gate, (((1,), (1,)), ((), ())), preferred_element_type=jnp.float32
    )
    input_summed = lax.psum_scatter(input_part, "shard", scatter_dimension=0, tiled=True)
    total = lax.psum(local_count, "replica").astype(jnp.float32)
    summed_grad = lax.psum_scatter(
        lax.dot_general(
            inputs, gate_raw, (((0,), (0,)), ((), ())), preferred_element_type=jnp.float32
        ),
        "replica",
        scatter_dimension=0,
        tiled=True,
    )
    scale = jnp.float32(group_rows * replicas) / total
    group_scale = jnp.float32(group_rows) / total
    input_grad = (input_summed * scale).astype(jnp.bfloat16)
    up_grad = (up_part * scale).astype(jnp.bfloat16)
    return (input_grad, up_grad) + adamw(summed_grad * group_scale, master, moment, second)


def flip(index, bit):
    return index + bit - 2 * bit * lax.rem(lax.div(index, bit), 2)


def exchange_kernel(
    x_hbm, gate_hbm, up_hbm, hid_hbm, seg_hbm, dw_hbm, w_hbm, ma_hbm, mo_hbm, se_hbm,
    ig_o, ug_o, gs_o, xt_o, gb, ma_o, mo_o, se_o,
    xs_v, xc_v, xg, gate_v, up_v, hid_v, seg_ref, dw_ref, w_v, xs32, xc32, xq, xp, tw_ref, gp, g32, gr, upo,
    part, rs_1, rs_2, cnt, cntr, dsum, lsem, wsem, tsem, ssem, rsem, far_sem,
):
    r, s = lax.axis_index("replica"), lax.axis_index("shard")
    replicas = lax.axis_size("replica")
    core, side, across = flip(r, 1), flip(r, 2), flip(flip(r, 1), 2)
    near, mid, far = flip(s, 1), flip(s, 2), flip(s, 4)
    mid_far = flip(mid, 4)
    inner = lax.rem(lax.rem(lax.div(s, 2), 2) + lax.div(s, 4), 2)
    odd_core = lax.rem(r, 2)
    rows, width = gate_v.shape[0], xc_v.shape[1]
    quarter, tall = rows // QUARTERS, rows // 8
    chunk, span = gb.shape[2], part.shape[2]
    f32, bf16 = jnp.float32, jnp.bfloat16
    q = lax.rem(s, QUARTERS)

    def at_quarter(index):
        return pl.ds(pl.multiple_of(index * quarter, quarter), quarter)

    def columns(owner):
        return pl.ds(pl.multiple_of(owner * width, width), width)

    def load(src, dst, sem):
        copy = pltpu.make_async_copy(src, dst, sem)
        copy.start()
        return copy

    barrier = pltpu.get_barrier_semaphore()
    peers = [(core, s), (side, s), (across, s), (r, near), (r, mid)]
    for peer in peers:
        pl.semaphore_signal(barrier, inc=1, device_id=peer, device_id_type=MESH)

    @pl.when(inner == 1)
    def greet_inner():
        pl.semaphore_signal(barrier, inc=1, device_id=(r, mid_far), device_id_type=MESH)


    l_seg = load(seg_hbm, seg_ref, lsem.at[0])
    l_dw = load(dw_hbm, dw_ref, lsem.at[1])
    l_xs = load(x_hbm.at[at_quarter(q), columns(side)], xs_v.at[0], lsem.at[2])
    l_xa = load(x_hbm.at[at_quarter(q), columns(across)], xs_v.at[1], lsem.at[3])
    l_gate = load(gate_hbm, gate_v, lsem.at[4])
    l_hid = load(hid_hbm, hid_v, lsem.at[5])
    l_up = load(up_hbm, up_v, lsem.at[6])
    l_w = [
        load(w_hbm.at[pl.ds(c * span, span), :], w_v.at[pl.ds(c * span, span), :], wsem.at[c])
        for c in range(CHUNKS)
    ]
    l_xc = load(x_hbm.at[:, columns(core)], xc_v, lsem.at[7])
    l_xo = load(x_hbm.at[:, columns(r)], xg.at[pl.ds(0, rows), :], lsem.at[8])
    started, by_odd, made = [], [], []

    def make(src, dst, peer, kept):
        k = len(made)
        copy = pltpu.make_async_remote_copy(
            src_ref=src, dst_ref=dst, send_sem=ssem.at[k], recv_sem=rsem.at[k],
            device_id=peer, device_id_type=MESH,
        )
        made.append(copy)
        kept.append(copy)
        return copy

    def push(src, dst, peer):
        copy = make(src, dst, peer, started)
        copy.start()
        return copy

    def when_odd(action):
        pl.when(odd_core == 1)(action)

    def when_even(action):
        pl.when(odd_core == 0)(action)

    l_seg.wait()
    l_dw.wait()
    docs = dw_ref.shape[1]
    seg = jnp.broadcast_to(seg_ref[...].astype(f32), (128, rows)).T[:, :docs]
    labels = lax.broadcasted_iota(jnp.int32, (rows, docs), 1).astype(f32)
    dw = jnp.broadcast_to(dw_ref[...].astype(f32), (rows, docs))
    tw = jnp.sum(jnp.where(seg == labels, dw, 0.0), axis=1, keepdims=True)
    tw_ref[...] = jnp.broadcast_to(tw, tw_ref.shape)
    cnt[...] = jnp.broadcast_to(jnp.sum(tw, axis=0, keepdims=True), cnt.shape)

    l_xs.wait()
    xs32[0] = xs_v[0].astype(f32)
    l_xa.wait()
    xs32[1] = xs_v[1].astype(f32)
    pl.semaphore_wait(barrier, len(peers) + inner)
    counts = [push(cnt, cntr.at[n], (peer, s)) for n, peer in enumerate((core, side, across))]
    x_first = [push(xs32.at[0], xq.at[0, 0], (side, s)), push(xs32.at[1], xq.at[1, 0], (across, s))]

    for copy in (l_gate, l_hid, l_up):
        copy.wait()
    g_side, g_core = [], []
    for k in range(CHUNKS):
        for j in range(chunk // 128):
            at, to = pl.ds(k * chunk + j * 128, 128), pl.ds(j * 128, 128)
            g = gate_v[:, at].astype(f32)
            sig = jax.nn.sigmoid(g)
            h = hid_v[:, at].astype(f32) * tw_ref[...]
            raw = (h * up_v[:, at].astype(f32) * sig * (1.0 + g * (1.0 - sig))).astype(bf16)
            upo[:, at] = h * g * sig
            gb[k, pl.ds(0, rows), to] = raw
            g32[k, :, to] = raw.astype(f32)
        if k < CHUNKS - LATE:
            g_side.append(push(g32.at[k], gr.at[1, k], (side, s)))
        else:
            g_side.append(make(g32.at[k], gr.at[1, k], (side, s), by_odd))
            when_odd(g_side[k].start)
        g_core.append(push(g32.at[k], gr.at[0, k], (core, s)))

    for n, position in enumerate(LAYOUT):
        block = s
        for bit in (1, 2, 4):
            if position & bit:
                block = flip(block, bit)
        at = pl.ds(pl.multiple_of(block * tall, tall), tall)
        for k in range(CHUNKS):
            gp[pl.ds(n * tall, tall), pl.ds(k * chunk, chunk)] = gb[k, at, :]

    first, second, states = {}, {}, {}

    def block(c, position):
        return part.at[c, pl.ds(LAYOUT.index(position) * tall, tall), :]

    def first_dim(c):
        return ((r, mid), 2) if KINDS[c] == "m" else ((r, near), 1)

    def second_dim(c):
        return ((r, near), 1) if KINDS[c] == "m" else ((r, mid), 2)

    def send_first(c, n):
        peer, bit = first_dim(c)
        position = bit + ((7 - bit, 3 - bit, 4, 0)[n])
        first[c, n] = push(block(c, position), rs_1.at[c, n], peer)

    def project(c):
        l_w[c].wait()
        part[c] = lax.dot_general(
            gp[...], w_v[pl.ds(c * span, span), :], (((1,), (1,)), ((), ())), preferred_element_type=f32
        )
        send_first(c, 0)

    def fetch(k):
        at = pl.ds(k * chunk, chunk)
        states[k] = [
            load(old.at[:, at], new.at[k], tsem.at[3 * k + n])
            for n, (old, new) in enumerate(((mo_hbm, mo_o), (se_hbm, se_o), (ma_hbm, ma_o)))
        ]

    def step_xc():
        l_xc.wait()
        xc32[...] = xc_v[...].astype(f32)
        x_core.append(push(xc32, xp, (core, s)))

    def forward(c, n):
        peer, bit = second_dim(c)
        kept = block(c, bit + 4 * (1 - n))
        first[c, n].wait_recv()
        kept[...] = kept[...] + rs_1[c, n]
        second[c, n] = push(kept, rs_2.at[c, n], peer)

    def open_far():
        pl.semaphore_wait(far_sem, 1)

    def announce():
        @pl.when(inner == 1)
        def tell():
            for peer in ((r, mid), (r, mid_far)):
                pl.semaphore_signal(far_sem, inc=1, device_id=peer, device_id_type=MESH)

    def forward_far(c):
        kept = block(c, 4)
        first[c, 2].wait_recv()
        second[c, 0].wait_recv()
        kept[...] = kept[...] + rs_1[c, 2] + rs_2[c, 0]
        second[c, 2] = push(kept, rs_2.at[c, 2], (r, far))

    def finish(c):
        first[c, 3].wait_recv()
        total = block(c, 0)[...] + rs_1[c, 3]
        for n in (1, 2):
            second[c, n].wait_recv()
            total = total + rs_2[c, n]
        ig_o[:, pl.ds(c * span, span)] = (total * scale[0]).astype(bf16)

    def keep_x(group, slot, index):
        to = pl.ds(pl.multiple_of((group + 2) * rows + index * quarter, quarter), quarter)
        xg[to, :] = xq[group, slot].astype(bf16)

    def turn(group):
        xt_o[:, pl.ds(group * rows, rows)] = xg[pl.ds(group * rows, rows), :].T

    def step_x(group):
        x_first[group].wait_recv()
        x_near[group] = push(xq.at[group, 0], xq.at[group, 1], (r, near))
        x_mid[group] = push(xq.at[group, 0], xq.at[group, 2], (r, mid))
        keep_x(group, 0, q)

    def step_x_last(group):
        if X_LAST[group] == "mid":
            x_near[group].wait_recv()
            x_last[group] = push(xq.at[group, 1], xq.at[group, 3], (r, mid))
        else:
            x_mid[group].wait_recv()
            x_last[group] = push(xq.at[group, 2], xq.at[group, 3], (r, near))

    def step_x_end(group):
        if X_LAST[group] == "mid":
            x_mid[group].wait_recv()
        else:
            x_near[group].wait_recv()
        x_last[group].wait_recv()
        keep_x(group, 1, lax.rem(near, QUARTERS))
        keep_x(group, 2, lax.rem(mid, QUARTERS))
        keep_x(group, 3, lax.rem(flip(near, 2), QUARTERS))
        turn(group + 2)

    def step_own():
        l_xo.wait()
        turn(0)
        x_core[0].wait_recv()
        xg[pl.ds(rows, rows), :] = xp[...].astype(bf16)
        turn(1)

    def store_g(k, group):
        value = gr[group, k].astype(bf16)
        gb[k, pl.ds((group + 1) * rows, rows), :] = value

    def step_core():
        for k in range(CHUNKS):
            if k < CHUNKS - LATE:
                g_core[k].wait_recv()
            else:
                when_even(g_core[k].wait_recv)
            store_g(k, 0)

    def lend():
        for k in range(CHUNKS - LATE, CHUNKS):
            g_lent[k] = make(gr.at[0, k], gr.at[2, k], (side, s), by_odd)
            g_across[k] = make(gr.at[1, k], gr.at[2, k], (core, s), by_odd)
            g_back[k] = make(gr.at[2, k], gr.at[1, k], (core, s), by_odd)

        def send():
            for k in range(CHUNKS - LATE, CHUNKS):
                g_core[k].wait_recv()
                g_lent[k].start()

        when_odd(send)

    def relay(k):
        if k >= CHUNKS - LATE:
            def both():
                g_side[k].wait_recv()
                g_across[k].start()
                g_lent[k].wait_recv()
                g_back[k].start()
                store_g(k, 1)
                store_g(k, 2)

            when_odd(both)
            return
        g_side[k].wait_recv()
        g_across[k] = push(gr.at[1, k], gr.at[2, k], (core, s))
        store_g(k, 1)

    def step_scale():
        for copy in counts:
            copy.wait_recv()
        total = (cnt[...] + cntr[0] + cntr[1] + cntr[2])[0:1, 0:1]
        scale.append(f32(rows * replicas) / total)
        scale.append(f32(rows) / total)
        gs_o[...] = jnp.broadcast_to(scale[1], gs_o.shape)
        ug_o[...] = (upo[...] * scale[0]).astype(bf16)

    def take(k):
        if k >= CHUNKS - LATE:
            def both():
                g_across[k].wait_recv()
                g_back[k].wait_recv()
                store_g(k, 1)
                store_g(k, 2)

            when_even(both)
            return
        g_across[k].wait_recv()
        store_g(k, 2)

    def optimize(k):
        dsum[...] = jnp.dot(xt_o[...], gb[k], preferred_element_type=f32)
        for copy in states[k]:
            copy.wait()
        for n in range(width // BAND):
            at = pl.ds(n * BAND, BAND)
            update(dsum[at, :] * scale[1], ma_o.at[k, at], mo_o.at[k, at], se_o.at[k, at],
                   ma_o.at[k, at], mo_o.at[k, at], se_o.at[k, at])

    x_core, x_near, x_mid, x_last, g_across, g_lent, g_back, scale = [], {}, {}, {}, {}, {}, {}, []
    steps = {
        "xc": step_xc, "own": step_own, "core": step_core, "scale": step_scale, "x": step_x, "xl": step_x_last,
        "xe": step_x_end, "st": fetch, "p": project, "lend": lend, "tell": announce, "far": open_far,
        "b": lambda c: send_first(c, 1), "c": lambda c: send_first(c, 2), "d": lambda c: send_first(c, 3),
        "a": lambda c: forward(c, 0), "e": lambda c: forward(c, 1), "f": forward_far, "i": finish, "g": relay, "t": take, "opt": optimize,
    }
    for name in ORDER:
        kind = name.rstrip("0123456789")
        index = name[len(kind):]
        steps[kind](*([int(index)] if index else []))
    for k in range(DONE, CHUNKS):
        for copy in states[k]:
            copy.wait()
    for copy in started:
        copy.wait_send()

    def wait_odd():
        for copy in by_odd:
            copy.wait_send()

    when_odd(wait_odd)


def update(grad, ma, mo, se, ma_to, mo_to, se_to):
    moment_new = 0.9 * mo[...] + 0.1 * grad
    second_new = 0.95 * se[...] + 0.05 * grad * grad
    master = ma[...]
    mo_to[...] = moment_new
    se_to[...] = second_new
    first_fix = moment_new * (1.0 / (1.0 - 0.9**8))
    second_fix = second_new * (1.0 / (1.0 - 0.95**8))
    ma_to[...] = master - 0.003 * (first_fix / (jnp.sqrt(second_fix) + 1e-08) + 0.1 * master)


def exchange(inputs, gate_pre, up_pre, hidden_grad, segment_ids, doc_weight, w_gate, master, moment, second):
    replicas, shards = lax.axis_size("replica"), lax.axis_size("shard")
    rows, features = inputs.shape
    hidden = gate_pre.shape[1]
    width, tall, quarter = features // replicas, rows // shards, rows // QUARTERS
    chunk, span = hidden // CHUNKS, features // CHUNKS
    f32, bf16 = jnp.float32, jnp.bfloat16
    hbm = pl.BlockSpec(memory_space=pltpu.HBM)
    vmem = pl.BlockSpec(memory_space=pltpu.VMEM)
    copies = 2 + 3 + 2 * CHUNKS + 1 + 6 + CHUNKS + 7 * CHUNKS + 2 * LATE
    state = pltpu.VMEM((CHUNKS, width, chunk), f32)
    operands = (inputs, gate_pre, up_pre, hidden_grad, segment_ids, doc_weight, w_gate, master, moment, second)
    return pl.pallas_call(
        exchange_kernel,
        out_shape=(
            pltpu.VMEM((tall, features), bf16),
            pltpu.VMEM((rows, hidden), bf16),
            pltpu.VMEM((8, chunk), f32),
            pltpu.VMEM((width, replicas * rows), bf16),
            pltpu.VMEM((CHUNKS, replicas * rows, chunk), bf16),
            state,
            state,
            state,
        ),
        in_specs=[hbm] * 10,
        out_specs=(vmem,) * 8,
        scratch_shapes=[
            pltpu.VMEM((2, quarter, width), bf16),
            pltpu.VMEM((rows, width), bf16),
            pltpu.VMEM((replicas * rows, width), bf16),
            pltpu.VMEM((rows, hidden), bf16),
            pltpu.VMEM((rows, hidden), bf16),
            pltpu.VMEM((rows, hidden), bf16),
            pltpu.VMEM(segment_ids.shape, jnp.int32),
            pltpu.VMEM(doc_weight.shape, jnp.int32),
            pltpu.VMEM((features, hidden), bf16),
            pltpu.VMEM((2, quarter, width), f32),
            pltpu.VMEM((rows, width), f32),
            pltpu.VMEM((2, QUARTERS, quarter, width), f32),
            pltpu.VMEM((rows, width), f32),
            pltpu.VMEM((rows, 128), f32),
            pltpu.VMEM((rows, hidden), bf16),
            pltpu.VMEM((CHUNKS, rows, chunk), f32),
            pltpu.VMEM((3, CHUNKS, rows, chunk), f32),
            pltpu.VMEM((rows, hidden), f32),
            pltpu.VMEM((CHUNKS, rows, span), f32),
            pltpu.VMEM((CHUNKS, 4, tall, span), f32),
            pltpu.VMEM((CHUNKS, 3, tall, span), f32),
            pltpu.VMEM((8, 128), f32),
            pltpu.VMEM((3, 8, 128), f32),
            pltpu.VMEM((width, chunk), f32),
            pltpu.SemaphoreType.DMA((9,)),
            pltpu.SemaphoreType.DMA((CHUNKS,)),
            pltpu.SemaphoreType.DMA((3 * CHUNKS,)),
            pltpu.SemaphoreType.DMA((copies,)),
            pltpu.SemaphoreType.DMA((copies,)),
            pltpu.SemaphoreType.REGULAR,
        ],
        compiler_params=pltpu.CompilerParams(
            collective_id=0, has_side_effects=True, vmem_limit_bytes=40 * 1024 * 1024
        ),
        cost_estimate=pl.CostEstimate(
            flops=4 * rows * hidden * features, bytes_accessed=12 * 1024 * 1024, transcendentals=0
        ),
        name="exchange",
    )(*[pltpu.with_memory_space_constraint(operand, pltpu.HBM) for operand in operands])


def step_kernel(
    ig_ref, ug_ref, gs_ref, xt_ref, gb_ref, ma_ref, mo_ref, se_ref,
    ig_hbm, ug_hbm, ma_hbm, mo_hbm, se_hbm,
    ma_v, mo_v, se_v, sems,
):
    written = []
    chunks, width, chunk = ma_ref.shape

    def write(src, dst):
        copy = pltpu.make_async_copy(src, dst, sems.at[len(written)])
        copy.start()
        written.append(copy)

    for k in range(DONE):
        for src, dst in ((mo_ref, mo_hbm), (se_ref, se_hbm), (ma_ref, ma_hbm)):
            write(src.at[k], dst.at[:, pl.ds(k * chunk, chunk)])
    write(ig_ref, ig_hbm)
    write(ug_ref, ug_hbm)
    group_scale = gs_ref[0:1, :]
    half = width // 2
    for k in range(DONE, chunks):
        for m in range(2):
            rows = pl.ds(m * half, half)
            raw = jnp.dot(xt_ref[rows, :], gb_ref[k], preferred_element_type=jnp.float32)
            mo_v[k - DONE, rows, :] = raw * group_scale
            for n in range(half // BAND):
                at = pl.ds(m * half + n * BAND, BAND)
                update(mo_v[k - DONE, at, :], ma_ref.at[k, at], mo_ref.at[k, at], se_ref.at[k, at],
                       ma_v.at[k - DONE, at], mo_v.at[k - DONE, at], se_v.at[k - DONE, at])
            for src, dst in ((mo_v, mo_hbm), (se_v, se_hbm), (ma_v, ma_hbm)):
                write(src.at[k - DONE, rows], dst.at[rows, pl.ds(k * chunk, chunk)])
    for copy in written:
        copy.wait()


def step(ig, ug, gs, xt, gb, ma, mo, se):
    chunks, width, chunk = ma.shape
    f32 = jnp.float32
    hbm = pl.BlockSpec(memory_space=pltpu.HBM)
    vmem = pl.BlockSpec(memory_space=pltpu.VMEM)
    late = pltpu.VMEM((chunks - DONE, width, chunk), f32)
    return pl.pallas_call(
        step_kernel,
        out_shape=(
            jax.ShapeDtypeStruct(ig.shape, ig.dtype),
            jax.ShapeDtypeStruct(ug.shape, ug.dtype),
        )
        + (jax.ShapeDtypeStruct((width, chunks * chunk), f32),) * 3,
        in_specs=[vmem] * 8,
        out_specs=(hbm,) * 5,
        scratch_shapes=[late, late, late, pltpu.SemaphoreType.DMA((2 + 3 * DONE + 6 * (chunks - DONE),))],
        compiler_params=pltpu.CompilerParams(vmem_limit_bytes=40 * 1024 * 1024),
        name="step",
    )(ig, ug, gs, xt, gb, ma, mo, se)


def gather_path(*args):
    return step(*exchange(*args))


def on_device(*args):
    inputs, gate_pre = args[:2]
    replicas, shards = lax.axis_size("replica"), lax.axis_size("shard")
    rows, features = inputs.shape
    hidden = gate_pre.shape[1]
    gathered = replicas * rows * (features // replicas + hidden)
    fits = rows % (QUARTERS * 32) == 0 and features % (replicas * 128) == 0 and hidden % (CHUNKS * 128) == 0
    if (replicas, shards) == (4, 8) and fits and gathered <= features * hidden:
        return gather_path(*args)
    return reduce_path(*args)


def solution(mesh):
    in_specs = (
        P("replica", None),
        P("replica", "shard"),
        P("replica", "shard"),
        P("replica", "shard"),
        P("replica", None),
        P("replica", None),
        P(None, "shard"),
        P("replica", "shard"),
        P("replica", "shard"),
        P("replica", "shard"),
    )
    out_specs = (
        P(("replica", "shard"), None),
        P("replica", "shard"),
        P("replica", "shard"),
        P("replica", "shard"),
        P("replica", "shard"),
    )
    return jax.shard_map(
        on_device, mesh=mesh, in_specs=in_specs, out_specs=out_specs, check_vma=False
    )
```

```python
import functools

import jax
import jax.numpy as jnp
from jax import lax
from jax.experimental import pallas as pl
from jax.experimental.pallas import tpu as pltpu
from jax.sharding import PartitionSpec as P

MESH = pl.DeviceIdType.MESH
QUARTERS = 4
CHUNKS = 4
BAND = 64
LAYOUT = (7, 3, 5, 1, 6, 2, 4, 0)
KINDS = "mhmh"
X_LAST = ("near", "near")
DONE = 3
ORDER = (
    "p0", "pass", "p1", "xc", "c0", "p3", "p2", "st0", "st1", "st2", "st3", "c2", "b3", "c1", "b2",
    "b1", "a0", "x1", "a1", "a2", "x0", "b0", "c3", "a3", "e1", "far", "f1", "core", "d0", "scale",
    "e3", "d2", "own", "f0", "xl1", "f2", "g0", "xl0", "d3", "d1", "g1", "f3", "e0", "e2", "xe1",
    "t1", "g2", "xe0", "t0", "opt1", "t2", "g3", "opt2", "opt0", "i1", "i0", "i2", "i3", "t3",
)


def token_weights(segment_ids, doc_weight):
    labels = jnp.arange(doc_weight.shape[1], dtype=jnp.int32)
    onehot = segment_ids[:, :, None] == labels[None, None, :]
    return jnp.sum(jnp.where(onehot, doc_weight[:, None, :], 0), axis=2)


def adamw(grad, master, moment, second):
    moment_new = 0.9 * moment + 0.1 * grad
    second_new = 0.95 * second + 0.05 * grad * grad
    first_fix = moment_new / (1.0 - 0.9**8)
    second_fix = second_new / (1.0 - 0.95**8)
    master_new = master - 0.003 * (first_fix / (jnp.sqrt(second_fix) + 1e-08) + 0.1 * master)
    return master_new, moment_new, second_new


def reduce_path(
    inputs, gate_pre, up_pre, hidden_grad, segment_ids, doc_weight, w_gate, master, moment, second
):
    group_rows = inputs.shape[0]
    replicas = lax.axis_size("replica")
    weights = token_weights(segment_ids, doc_weight)[0]
    local_count = jnp.sum(weights)
    gate_f = gate_pre.astype(jnp.float32)
    sigmoid_gate = jax.nn.sigmoid(gate_f)
    weighted = hidden_grad.astype(jnp.float32) * weights.astype(jnp.float32)[:, None]
    gate_raw = (
        weighted * up_pre.astype(jnp.float32) * sigmoid_gate * (1.0 + gate_f * (1.0 - sigmoid_gate))
    ).astype(jnp.bfloat16)
    up_part = weighted * gate_f * sigmoid_gate
    input_part = lax.dot_general(
        gate_raw, w_gate, (((1,), (1,)), ((), ())), preferred_element_type=jnp.float32
    )
    input_summed = lax.psum_scatter(input_part, "shard", scatter_dimension=0, tiled=True)
    total = lax.psum(local_count, "replica").astype(jnp.float32)
    summed_grad = lax.psum_scatter(
        lax.dot_general(
            inputs, gate_raw, (((0,), (0,)), ((), ())), preferred_element_type=jnp.float32
        ),
        "replica",
        scatter_dimension=0,
        tiled=True,
    )
    scale = jnp.float32(group_rows * replicas) / total
    group_scale = jnp.float32(group_rows) / total
    input_grad = (input_summed * scale).astype(jnp.bfloat16)
    up_grad = (up_part * scale).astype(jnp.bfloat16)
    return (input_grad, up_grad) + adamw(summed_grad * group_scale, master, moment, second)


def flip(index, bit):
    return index + bit - 2 * bit * lax.rem(lax.div(index, bit), 2)


def exchange_kernel(
    x_hbm, gate_hbm, up_hbm, hid_hbm, seg_hbm, dw_hbm, w_hbm, ma_hbm, mo_hbm, se_hbm,
    ig_o, ug_o, gs_o, xt_o, gb, ma_o, mo_o, se_o,
    xs_v, xc_v, xg, gate_v, up_v, hid_v, seg_ref, dw_ref, w_v, xs32, xc32, xq, xp, tw_ref, gp, g32, gr, upo,
    part, rs_1, rs_2, cnt, cntr, dsum, lsem, wsem, tsem, ssem, rsem, both_sem, near_sem, far_sem,
):
    r, s = lax.axis_index("replica"), lax.axis_index("shard")
    replicas = lax.axis_size("replica")
    core, side, across = flip(r, 1), flip(r, 2), flip(flip(r, 1), 2)
    near, mid, far = flip(s, 1), flip(s, 2), flip(s, 4)
    mid_far = flip(mid, 4)
    odd_core = lax.rem(r, 2)
    inner = lax.rem(lax.rem(lax.div(s, 2), 2) + lax.div(s, 4), 2)
    rows, width = gate_v.shape[0], xc_v.shape[1]
    quarter, tall = rows // QUARTERS, rows // 8
    chunk, span = gb.shape[2], part.shape[2]
    f32, bf16 = jnp.float32, jnp.bfloat16
    q = lax.rem(s, QUARTERS)

    def at_quarter(index):
        return pl.ds(pl.multiple_of(index * quarter, quarter), quarter)

    def columns(owner):
        return pl.ds(pl.multiple_of(owner * width, width), width)

    def load(src, dst, sem):
        copy = pltpu.make_async_copy(src, dst, sem)
        copy.start()
        return copy

    barrier = pltpu.get_barrier_semaphore()
    peers = [(core, s), (side, s), (across, s)]
    for peer in peers:
        pl.semaphore_signal(barrier, inc=1, device_id=peer, device_id_type=MESH)

    @pl.when(odd_core == 1)
    def greet_neighbours():
        for peer in ((r, near), (r, mid)):
            pl.semaphore_signal(barrier, inc=1, device_id=peer, device_id_type=MESH)

    @pl.when(odd_core * inner == 1)
    def greet_inner():
        pl.semaphore_signal(barrier, inc=1, device_id=(r, mid_far), device_id_type=MESH)

    l_seg = load(seg_hbm, seg_ref, lsem.at[0])
    l_dw = load(dw_hbm, dw_ref, lsem.at[1])
    l_xs = load(x_hbm.at[at_quarter(q), columns(side)], xs_v.at[0], lsem.at[2])
    l_xa = load(x_hbm.at[at_quarter(q), columns(across)], xs_v.at[1], lsem.at[3])
    l_gate = load(gate_hbm, gate_v, lsem.at[4])
    l_hid = load(hid_hbm, hid_v, lsem.at[5])
    l_up = load(up_hbm, up_v, lsem.at[6])
    l_w = [
        load(w_hbm.at[pl.ds(c * span, span), :], w_v.at[pl.ds(c * span, span), :], wsem.at[c])
        for c in range(CHUNKS)
    ]
    l_xc = load(x_hbm.at[:, columns(core)], xc_v, lsem.at[7])
    l_xo = load(x_hbm.at[:, columns(r)], xg.at[pl.ds(0, rows), :], lsem.at[8])
    started = []

    def push(src, dst, peer):
        k = len(started)
        copy = pltpu.make_async_remote_copy(
            src_ref=src, dst_ref=dst, send_sem=ssem.at[k], recv_sem=rsem.at[k],
            device_id=peer, device_id_type=MESH,
        )
        copy.start()
        started.append(copy)
        return copy

    l_seg.wait()
    l_dw.wait()
    docs = dw_ref.shape[1]
    seg = jnp.broadcast_to(seg_ref[...].astype(f32), (128, rows)).T[:, :docs]
    labels = lax.broadcasted_iota(jnp.int32, (rows, docs), 1).astype(f32)
    dw = jnp.broadcast_to(dw_ref[...].astype(f32), (rows, docs))
    tw = jnp.sum(jnp.where(seg == labels, dw, 0.0), axis=1, keepdims=True)
    tw_ref[...] = jnp.broadcast_to(tw, tw_ref.shape)
    cnt[...] = jnp.broadcast_to(jnp.sum(tw, axis=0, keepdims=True), cnt.shape)

    l_xs.wait()
    xs32[0] = xs_v[0].astype(f32)
    l_xa.wait()
    xs32[1] = xs_v[1].astype(f32)
    pl.semaphore_wait(barrier, len(peers) + odd_core * (2 + inner))
    counts = [push(cnt, cntr.at[n], (peer, s)) for n, peer in enumerate((core, side, across))]
    x_first = [push(xs32.at[0], xq.at[0, 0], (side, s)), push(xs32.at[1], xq.at[1, 0], (across, s))]

    @pl.when(odd_core == 1)
    def tell_both_in():
        for peer in ((r, near), (r, mid)):
            pl.semaphore_signal(both_sem, inc=1, device_id=peer, device_id_type=MESH)

    @pl.when(odd_core * inner == 1)
    def tell_both_in_inner():
        pl.semaphore_signal(both_sem, inc=1, device_id=(r, mid_far), device_id_type=MESH)

    for copy in (l_gate, l_hid, l_up):
        copy.wait()
    g_side, g_core = [], []
    for k in range(CHUNKS):
        for j in range(chunk // 128):
            at, to = pl.ds(k * chunk + j * 128, 128), pl.ds(j * 128, 128)
            g = gate_v[:, at].astype(f32)
            sig = jax.nn.sigmoid(g)
            h = hid_v[:, at].astype(f32) * tw_ref[...]
            raw = (h * up_v[:, at].astype(f32) * sig * (1.0 + g * (1.0 - sig))).astype(bf16)
            upo[:, at] = h * g * sig
            gb[k, pl.ds(0, rows), to] = raw
            g32[k, :, to] = raw.astype(f32)
        g_side.append(push(g32.at[k], gr.at[1, k], (side, s)))
        g_core.append(push(g32.at[k], gr.at[0, k], (core, s)))

    for n, position in enumerate(LAYOUT):
        block = s
        for bit in (1, 2, 4):
            if position & bit:
                block = flip(block, bit)
        at = pl.ds(pl.multiple_of(block * tall, tall), tall)
        for k in range(CHUNKS):
            gp[pl.ds(n * tall, tall), pl.ds(k * chunk, chunk)] = gb[k, at, :]

    first, second, states = {}, {}, {}

    def block(c, position):
        return part.at[c, pl.ds(LAYOUT.index(position) * tall, tall), :]

    def first_dim(c):
        return ((r, mid), 2) if KINDS[c] == "m" else ((r, near), 1)

    def second_dim(c):
        return ((r, near), 1) if KINDS[c] == "m" else ((r, mid), 2)

    def send_first(c, n):
        peer, bit = first_dim(c)
        position = bit + ((7 - bit, 3 - bit, 4, 0)[n])
        first[c, n] = push(block(c, position), rs_1.at[c, n], peer)

    def project(c):
        l_w[c].wait()
        part[c] = lax.dot_general(
            gp[...], w_v[pl.ds(c * span, span), :], (((1,), (1,)), ((), ())), preferred_element_type=f32
        )
        if not first:
            open_near()
        send_first(c, 0)

    def fetch(k):
        at = pl.ds(k * chunk, chunk)
        states[k] = [
            load(old.at[:, at], new.at[k], tsem.at[3 * k + n])
            for n, (old, new) in enumerate(((mo_hbm, mo_o), (se_hbm, se_o), (ma_hbm, ma_o)))
        ]

    def step_xc():
        l_xc.wait()
        xc32[...] = xc_v[...].astype(f32)
        x_core.append(push(xc32, xp, (core, s)))

    def forward(c, n):
        peer, bit = second_dim(c)
        kept = block(c, bit + 4 * (1 - n))
        first[c, n].wait_recv()
        kept[...] = kept[...] + rs_1[c, n]
        second[c, n] = push(kept, rs_2.at[c, n], peer)

    def open_near():
        @pl.when(odd_core == 0)
        def hear():
            pl.semaphore_wait(near_sem, 1)

    def pass_near():
        @pl.when(odd_core == 1)
        def hear():
            pl.semaphore_wait(both_sem, 2 + inner)
            pl.semaphore_signal(near_sem, inc=1, device_id=(core, s), device_id_type=MESH)

        @pl.when(odd_core * inner == 1)
        def tell():
            for peer in ((r, mid), (r, mid_far)):
                pl.semaphore_signal(far_sem, inc=1, device_id=peer, device_id_type=MESH)

    def open_far():
        pl.semaphore_wait(far_sem, 1)

        @pl.when(odd_core == 1)
        def tell():
            pl.semaphore_signal(far_sem, inc=1, device_id=(core, s), device_id_type=MESH)

    def forward_far(c):
        kept = block(c, 4)
        first[c, 2].wait_recv()
        second[c, 0].wait_recv()
        kept[...] = kept[...] + rs_1[c, 2] + rs_2[c, 0]
        second[c, 2] = push(kept, rs_2.at[c, 2], (r, far))

    def finish(c):
        first[c, 3].wait_recv()
        total = block(c, 0)[...] + rs_1[c, 3]
        for n in (1, 2):
            second[c, n].wait_recv()
            total = total + rs_2[c, n]
        ig_o[:, pl.ds(c * span, span)] = (total * scale[0]).astype(bf16)

    def keep_x(group, slot, index):
        to = pl.ds(pl.multiple_of((group + 2) * rows + index * quarter, quarter), quarter)
        xg[to, :] = xq[group, slot].astype(bf16)

    def turn(group):
        xt_o[:, pl.ds(group * rows, rows)] = xg[pl.ds(group * rows, rows), :].T

    def step_x(group):
        x_first[group].wait_recv()
        x_near[group] = push(xq.at[group, 0], xq.at[group, 1], (r, near))
        x_mid[group] = push(xq.at[group, 0], xq.at[group, 2], (r, mid))
        keep_x(group, 0, q)

    def step_x_last(group):
        if X_LAST[group] == "mid":
            x_near[group].wait_recv()
            x_last[group] = push(xq.at[group, 1], xq.at[group, 3], (r, mid))
        else:
            x_mid[group].wait_recv()
            x_last[group] = push(xq.at[group, 2], xq.at[group, 3], (r, near))

    def step_x_end(group):
        if X_LAST[group] == "mid":
            x_mid[group].wait_recv()
        else:
            x_near[group].wait_recv()
        x_last[group].wait_recv()
        keep_x(group, 1, lax.rem(near, QUARTERS))
        keep_x(group, 2, lax.rem(mid, QUARTERS))
        keep_x(group, 3, lax.rem(flip(near, 2), QUARTERS))
        turn(group + 2)

    def step_own():
        l_xo.wait()
        turn(0)
        x_core[0].wait_recv()
        xg[pl.ds(rows, rows), :] = xp[...].astype(bf16)
        turn(1)

    def store_g(k, group):
        value = gr[group, k].astype(bf16)
        gb[k, pl.ds((group + 1) * rows, rows), :] = value

    def step_core():
        for k in range(CHUNKS):
            g_core[k].wait_recv()
            store_g(k, 0)

    def relay(k):
        g_side[k].wait_recv()
        g_across[k] = push(gr.at[1, k], gr.at[2, k], (core, s))
        store_g(k, 1)

    def step_scale():
        for copy in counts:
            copy.wait_recv()
        total = (cnt[...] + cntr[0] + cntr[1] + cntr[2])[0:1, 0:1]
        scale.append(f32(rows * replicas) / total)
        scale.append(f32(rows) / total)
        gs_o[...] = jnp.broadcast_to(scale[1], gs_o.shape)
        ug_o[...] = (upo[...] * scale[0]).astype(bf16)

    def take(k):
        g_across[k].wait_recv()
        store_g(k, 2)

    def optimize(k):
        dsum[...] = jnp.dot(xt_o[...], gb[k], preferred_element_type=f32)
        for copy in states[k]:
            copy.wait()
        for n in range(width // BAND):
            at = pl.ds(n * BAND, BAND)
            update(dsum[at, :] * scale[1], ma_o.at[k, at], mo_o.at[k, at], se_o.at[k, at],
                   ma_o.at[k, at], mo_o.at[k, at], se_o.at[k, at])

    x_core, x_near, x_mid, x_last, g_across, scale = [], {}, {}, {}, {}, []
    steps = {
        "xc": step_xc, "own": step_own, "core": step_core, "scale": step_scale, "x": step_x, "xl": step_x_last,
        "xe": step_x_end, "st": fetch, "p": project, "pass": pass_near, "far": open_far,
        "b": lambda c: send_first(c, 1), "c": lambda c: send_first(c, 2), "d": lambda c: send_first(c, 3),
        "a": lambda c: forward(c, 0), "e": lambda c: forward(c, 1), "f": forward_far, "i": finish, "g": relay, "t": take, "opt": optimize,
    }
    for name in ORDER:
        kind = name.rstrip("0123456789")
        index = name[len(kind):]
        steps[kind](*([int(index)] if index else []))
    for k in range(DONE, CHUNKS):
        for copy in states[k]:
            copy.wait()
    for copy in started:
        copy.wait_send()


def update(grad, ma, mo, se, ma_to, mo_to, se_to):
    moment_new = 0.9 * mo[...] + 0.1 * grad
    second_new = 0.95 * se[...] + 0.05 * grad * grad
    master = ma[...]
    mo_to[...] = moment_new
    se_to[...] = second_new
    first_fix = moment_new * (1.0 / (1.0 - 0.9**8))
    second_fix = second_new * (1.0 / (1.0 - 0.95**8))
    ma_to[...] = master - 0.003 * (first_fix / (jnp.sqrt(second_fix) + 1e-08) + 0.1 * master)


def exchange(inputs, gate_pre, up_pre, hidden_grad, segment_ids, doc_weight, w_gate, master, moment, second):
    replicas, shards = lax.axis_size("replica"), lax.axis_size("shard")
    rows, features = inputs.shape
    hidden = gate_pre.shape[1]
    width, tall, quarter = features // replicas, rows // shards, rows // QUARTERS
    chunk, span = hidden // CHUNKS, features // CHUNKS
    f32, bf16 = jnp.float32, jnp.bfloat16
    hbm = pl.BlockSpec(memory_space=pltpu.HBM)
    vmem = pl.BlockSpec(memory_space=pltpu.VMEM)
    copies = 2 + 3 + 2 * CHUNKS + 1 + 6 + CHUNKS + 7 * CHUNKS
    state = pltpu.VMEM((CHUNKS, width, chunk), f32)
    operands = (inputs, gate_pre, up_pre, hidden_grad, segment_ids, doc_weight, w_gate, master, moment, second)
    return pl.pallas_call(
        exchange_kernel,
        out_shape=(
            pltpu.VMEM((tall, features), bf16),
            pltpu.VMEM((rows, hidden), bf16),
            pltpu.VMEM((8, chunk), f32),
            pltpu.VMEM((width, replicas * rows), bf16),
            pltpu.VMEM((CHUNKS, replicas * rows, chunk), bf16),
            state,
            state,
            state,
        ),
        in_specs=[hbm] * 10,
        out_specs=(vmem,) * 8,
        scratch_shapes=[
            pltpu.VMEM((2, quarter, width), bf16),
            pltpu.VMEM((rows, width), bf16),
            pltpu.VMEM((replicas * rows, width), bf16),
            pltpu.VMEM((rows, hidden), bf16),
            pltpu.VMEM((rows, hidden), bf16),
            pltpu.VMEM((rows, hidden), bf16),
            pltpu.VMEM(segment_ids.shape, jnp.int32),
            pltpu.VMEM(doc_weight.shape, jnp.int32),
            pltpu.VMEM((features, hidden), bf16),
            pltpu.VMEM((2, quarter, width), f32),
            pltpu.VMEM((rows, width), f32),
            pltpu.VMEM((2, QUARTERS, quarter, width), f32),
            pltpu.VMEM((rows, width), f32),
            pltpu.VMEM((rows, 128), f32),
            pltpu.VMEM((rows, hidden), bf16),
            pltpu.VMEM((CHUNKS, rows, chunk), f32),
            pltpu.VMEM((3, CHUNKS, rows, chunk), f32),
            pltpu.VMEM((rows, hidden), f32),
            pltpu.VMEM((CHUNKS, rows, span), f32),
            pltpu.VMEM((CHUNKS, 4, tall, span), f32),
            pltpu.VMEM((CHUNKS, 3, tall, span), f32),
            pltpu.VMEM((8, 128), f32),
            pltpu.VMEM((3, 8, 128), f32),
            pltpu.VMEM((width, chunk), f32),
            pltpu.SemaphoreType.DMA((9,)),
            pltpu.SemaphoreType.DMA((CHUNKS,)),
            pltpu.SemaphoreType.DMA((3 * CHUNKS,)),
            pltpu.SemaphoreType.DMA((copies,)),
            pltpu.SemaphoreType.DMA((copies,)),
            pltpu.SemaphoreType.REGULAR,
            pltpu.SemaphoreType.REGULAR,
            pltpu.SemaphoreType.REGULAR,
        ],
        compiler_params=pltpu.CompilerParams(
            collective_id=0, has_side_effects=True, vmem_limit_bytes=40 * 1024 * 1024
        ),
        cost_estimate=pl.CostEstimate(
            flops=4 * rows * hidden * features, bytes_accessed=12 * 1024 * 1024, transcendentals=0
        ),
        name="exchange",
    )(*[pltpu.with_memory_space_constraint(operand, pltpu.HBM) for operand in operands])


def step_kernel(
    ig_ref, ug_ref, gs_ref, xt_ref, gb_ref, ma_ref, mo_ref, se_ref,
    ig_hbm, ug_hbm, ma_hbm, mo_hbm, se_hbm,
    ma_v, mo_v, se_v, sems,
):
    written = []
    chunks, width, chunk = ma_ref.shape

    def write(src, dst):
        copy = pltpu.make_async_copy(src, dst, sems.at[len(written)])
        copy.start()
        written.append(copy)

    for k in range(DONE):
        for src, dst in ((mo_ref, mo_hbm), (se_ref, se_hbm), (ma_ref, ma_hbm)):
            write(src.at[k], dst.at[:, pl.ds(k * chunk, chunk)])
    write(ig_ref, ig_hbm)
    write(ug_ref, ug_hbm)
    group_scale = gs_ref[0:1, :]
    half = width // 2
    for k in range(DONE, chunks):
        for m in range(2):
            rows = pl.ds(m * half, half)
            raw = jnp.dot(xt_ref[rows, :], gb_ref[k], preferred_element_type=jnp.float32)
            mo_v[k - DONE, rows, :] = raw * group_scale
            for n in range(half // BAND):
                at = pl.ds(m * half + n * BAND, BAND)
                update(mo_v[k - DONE, at, :], ma_ref.at[k, at], mo_ref.at[k, at], se_ref.at[k, at],
                       ma_v.at[k - DONE, at], mo_v.at[k - DONE, at], se_v.at[k - DONE, at])
            for src, dst in ((mo_v, mo_hbm), (se_v, se_hbm), (ma_v, ma_hbm)):
                write(src.at[k - DONE, rows], dst.at[rows, pl.ds(k * chunk, chunk)])
    for copy in written:
        copy.wait()


def step(ig, ug, gs, xt, gb, ma, mo, se):
    chunks, width, chunk = ma.shape
    f32 = jnp.float32
    hbm = pl.BlockSpec(memory_space=pltpu.HBM)
    vmem = pl.BlockSpec(memory_space=pltpu.VMEM)
    late = pltpu.VMEM((chunks - DONE, width, chunk), f32)
    return pl.pallas_call(
        step_kernel,
        out_shape=(
            jax.ShapeDtypeStruct(ig.shape, ig.dtype),
            jax.ShapeDtypeStruct(ug.shape, ug.dtype),
        )
        + (jax.ShapeDtypeStruct((width, chunks * chunk), f32),) * 3,
        in_specs=[vmem] * 8,
        out_specs=(hbm,) * 5,
        scratch_shapes=[late, late, late, pltpu.SemaphoreType.DMA((2 + 3 * DONE + 6 * (chunks - DONE),))],
        compiler_params=pltpu.CompilerParams(vmem_limit_bytes=40 * 1024 * 1024),
        name="step",
    )(ig, ug, gs, xt, gb, ma, mo, se)


def gather_path(*args):
    return step(*exchange(*args))


def on_device(*args):
    inputs, gate_pre = args[:2]
    replicas, shards = lax.axis_size("replica"), lax.axis_size("shard")
    rows, features = inputs.shape
    hidden = gate_pre.shape[1]
    gathered = replicas * rows * (features // replicas + hidden)
    fits = rows % (QUARTERS * 32) == 0 and features % (replicas * 128) == 0 and hidden % (CHUNKS * 128) == 0
    if (replicas, shards) == (4, 8) and fits and gathered <= features * hidden:
        return gather_path(*args)
    return reduce_path(*args)


def solution(mesh):
    in_specs = (
        P("replica", None),
        P("replica", "shard"),
        P("replica", "shard"),
        P("replica", "shard"),
        P("replica", None),
        P("replica", None),
        P(None, "shard"),
        P("replica", "shard"),
        P("replica", "shard"),
        P("replica", "shard"),
    )
    out_specs = (
        P(("replica", "shard"), None),
        P("replica", "shard"),
        P("replica", "shard"),
        P("replica", "shard"),
        P("replica", "shard"),
    )
    return jax.shard_map(
        on_device, mesh=mesh, in_specs=in_specs, out_specs=out_specs, check_vma=False
    )
```
